32 devices in a mesh: blk: 32 (over z, y, x, core).
Axes of the slice: x: 2, y: 2, z: 4, core: 2. Of those that a mesh axis runs over, the one named last changes fastest.
Arguments:
- defect: float32 [384, 128], P('blk'), may hold values from -6 to 6
- mass: float32 [384, 128], P('blk'), may hold values from 1 to 2
- block_diag: float32 [384, 128, 128], P('blk'), may hold values from -0.1875 to 0.1875
- coupling: float32 [3072, 128, 128], P('blk'), may hold values from -0.09375 to 0.09375
- tile_rows: int32 [3072], P('blk'), may hold values from 0 to 383, as said below
- tile_cols: int32 [3072], P('blk'), may hold values from 0 to 383, as said below
Outputs:
- update: float32 [384, 128], P('blk')
The draws below stay inside these ranges and needn't reach their ends.
Inputs may be any that keep to these rules, and one draw needn't show every extreme that they name: `tile_rows`: block rows d * 12 to d * 12 + 11 belong to device d of blk, and each device holds the tiles at positions d * 96 to d * 96 + 95. Of every tile a device holds, exactly one of its block row and block column belongs to that device; the other belongs to a different device. Exactly half of the 96 tiles of every device have their block row with that device, and the other half their block column. A program may send only the blocks and products of tiles that exist; slots of a padded buffer that no tile fills need not be sent. `tile_cols`: of one device's tiles, at most 2 have their block column with any one other device and at most 2 have their block row with any one other device; every device reaches 2 with some other device on each of the two sides.
All inputs are finite; a program needn't handle non-finite values.
Results may differ from the reference program's by a relative error of at most 0.0001.
Values sent between devices are 32-bit elements; how exact they have to be, the bound alone decides.
No kernel may reach another device: no remote copies, remote signals or barrier semaphores. Data moves between devices by JAX's collectives and lax.ppermute only.
A program may use at most 64 MiB of HBM per device.

```python
import jax
import jax.numpy as jnp
from jax import lax

B = 128
K = 8
RB = 12
ITERS = 3
TD = 96
C = 2
NB = 384
NT = 3072
N_BLK = 32


def tile_pattern(key):
    base = jax.random.fold_in(key, 11)
    half = TD // 2
    peers = N_BLK - 1
    cells = peers * C
    antipode_lane = N_BLK // 2 - 1

    def one_device(device_key, device):
        keys = jax.random.split(device_key, 6)

        def pick(pick_key):
            order = jax.random.permutation(pick_key, cells).astype(jnp.int32)
            grid = jnp.arange(cells, dtype=jnp.int32)
            score = jnp.where(grid // C == antipode_lane, grid - cells, order)
            return (jnp.argsort(score, stable=True)[:half] // C).astype(jnp.int32)
        lanes = jnp.concatenate([pick(keys[1]), pick(keys[2])])
        far_device = (device + lanes + 1) % N_BLK
        own_slot = jax.random.randint(keys[3], (TD,), 0, RB).astype(jnp.int32)
        far_slot = jax.random.randint(keys[4], (TD,), 0, RB).astype(jnp.int32)
        own_block = device * RB + own_slot
        far_block = far_device * RB + far_slot
        first = jnp.arange(TD) < half
        rows = jnp.where(first, own_block, far_block)
        cols = jnp.where(first, far_block, own_block)
        shuffle = jax.random.permutation(keys[5], TD)
        return (rows[shuffle], cols[shuffle])
    owners = jnp.arange(N_BLK, dtype=jnp.int32)
    rows, cols = jax.vmap(one_device)(jax.random.split(base, N_BLK), owners)
    return (rows.reshape(NT).astype(jnp.int32), cols.reshape(NT).astype(jnp.int32))


def draw_tile_rows(key, part):
    return tile_pattern(key)[0]


def draw_tile_cols(key, part):
    return tile_pattern(key)[1]


def levels(rng, dims, cuts, least, top_value):
    def one(axis_at, blocks):
        steps = jax.random.uniform(jax.random.fold_in(jax.random.fold_in(rng, 6), axis_at), (blocks,), jnp.float32, least / len(cuts), top_value / len(cuts))
        return jnp.repeat(jnp.exp(steps), dims[axis_at] // blocks).reshape((-1,) + (1,) * (len(dims) - axis_at - 1))

    loudness = one(*cuts[0])
    for cut in cuts[1:]:
        loudness = loudness * one(*cut)
    return loudness


def gaussian(key, shape, scale, limit, cuts=(), held_as=jnp.bfloat16):
    drawn = jax.random.normal(key, shape, jnp.float32) * scale
    if len(cuts) > 0:
        drawn = levels(key, shape, cuts, -0.22, 0.18) * drawn
    return jnp.clip(drawn, min=-limit, max=limit).astype(held_as)


def setup_inputs(seed: int = 0) -> dict:
    splits = jax.random.split(jax.random.key(seed), 7)
    return {
        "defect": gaussian(splits[0], (NB, B), 1.0, 6.0, ((0, 32),), jnp.float32),
        "mass": jnp.clip(1.0 + 1.0 * jax.random.uniform(splits[1], (NB, B), jnp.float32) ** levels(splits[1], (NB, B), ((0, 32),), -0.2, 0.2), 1.0, 2.0),
        "block_diag": gaussian(splits[2], (NB, B, B), (8 * B) ** -0.5, 0.1875, ((0, 32),), jnp.float32),
        "coupling": gaussian(splits[3], (NT, B, B), (4 * K * B) ** -0.5, 0.09375, ((0, 32),), jnp.float32),
        "tile_rows": draw_tile_rows(jax.random.fold_in(splits[6], 71), 0),
        "tile_cols": draw_tile_cols(jax.random.fold_in(splits[6], 71), 0),
    }


def solve_small(gram, target):
    factor = jnp.linalg.cholesky(gram)
    count = gram.shape[0]
    forward = []
    for index in range(count):
        value = target[index]
        for inner in range(index):
            value = value - factor[index, inner] * forward[inner]
        forward.append(value / factor[index, index])
    backward = [None] * count
    for index in reversed(range(count)):
        value = forward[index]
        for inner in range(index + 1, count):
            value = value - factor[inner, index] * backward[inner]
        backward[index] = value / factor[index, index]
    return backward

def newton_apply(vector, mass, block_diag, coupling, tile_rows, tile_cols):
    own = jnp.einsum('rij,rj->ri', block_diag, vector, precision=lax.Precision.HIGHEST)
    products = jnp.einsum('tij,tj->ti', coupling, vector[tile_cols], precision=lax.Precision.HIGHEST)
    far = jax.ops.segment_sum(products, tile_rows, num_segments=NB)
    return mass * vector + own + far

def reference(defect, mass, block_diag, coupling, tile_rows, tile_cols):
    negated = -defect
    beta = jnp.sqrt(jnp.sum(negated * negated))
    basis = [negated / beta]
    upper = jnp.zeros((ITERS + 1, ITERS), jnp.float32)
    for column in range(ITERS):
        image = newton_apply(basis[column], mass, block_diag, coupling, tile_rows, tile_cols)
        dots = jnp.stack([jnp.sum(item * image) for item in basis])
        for index in range(column + 1):
            image = image - dots[index] * basis[index]
        norm = jnp.sqrt(jnp.sum(image * image))
        upper = upper.at[:column + 1, column].set(dots)
        upper = upper.at[column + 1, column].set(norm)
        if column + 1 < ITERS:
            basis.append(image / norm)
    gram = jnp.dot(upper.T.astype(jnp.float32), upper.astype(jnp.float32), precision=lax.Precision.HIGHEST, preferred_element_type=jnp.float32)
    mixing = solve_small(gram, beta * upper[0, :])
    update = jnp.zeros_like(defect)
    for index in range(ITERS):
        update = update + mixing[index] * basis[index]
    return update
```

```python
import functools

import jax
import jax.numpy as jnp
from jax import lax
from jax.experimental import pallas as pl
from jax.experimental.pallas import tpu as pltpu
from jax.sharding import PartitionSpec as P

F32 = jnp.float32
BF16 = jnp.bfloat16
NT = (((1,), (1,)), ((), ()))
NN = (((1,), (0,)), ((), ()))
TN = (((0,), (0,)), ((), ()))
FLOOR = 2.0**-22
MIB = 1 << 20


def round_up(value, step):
    return -(-value // step) * step


class Sizes:
    def __init__(self, devices, rows, width, tiles):
        self.devices = devices
        self.rows = rows
        self.width = width
        self.tiles = tiles
        self.half = tiles // 2
        self.slots = (self.half + devices - 2) // (devices - 1)
        self.padded = round_up(rows, 8)
        self.near = self.half + rows
        self.lanes = round_up(self.near, 64)
        self.first_rows = round_up(rows + self.slots + 1, 8)
        self.info_row = rows + self.slots
        self.send_rows = 2 * self.slots + 1


def dot(a, b, dims):
    return lax.dot_general(a, b, dims, preferred_element_type=F32)


def split(value):
    high = value.astype(BF16)
    low = (value - high.astype(F32)).astype(BF16)
    return high, low


def iota(shape, axis):
    return lax.broadcasted_iota(jnp.int32, shape, axis)


def fiota(shape, axis):
    return iota(shape, axis).astype(F32)


def total(value):
    return jnp.sum(jnp.sum(value, axis=0, keepdims=True), axis=1, keepdims=True)


def pick_rows(onehot, source):
    width = source.shape[1]
    high, low = split(source)
    out = dot(onehot, jnp.concatenate([high, low], axis=1), NN)
    return out[:, :width], out[:, width:]


def tile_inputs(pairs):
    high = low = None
    for onehot, source in pairs:
        h, l = pick_rows(onehot, source)
        high = h if high is None else high + h
        low = l if low is None else low + l
    return jnp.concatenate([high, low], axis=0).astype(BF16)


def place(result, acc, index, lanes):
    lane = iota(acc.shape, 1)
    return jnp.where((lane == index) | (lane == lanes + index), result, acc)


def tile_products(tiles_ref, count, inputs, lanes, group=4):
    width = inputs.shape[1]
    weights = jnp.concatenate([inputs, inputs], axis=1)
    acc = jnp.zeros((width, 2 * lanes), F32)
    for start in range(0, count, group):
        size = min(group, count - start)
        out = dot(tiles_ref[start * width : (start + size) * width, :], weights, NT)
        for inner in range(size):
            acc = place(out[inner * width : (inner + 1) * width], acc, start + inner, lanes)
    return acc


def sum_rows(select, products):
    high, low = split(products)
    return dot(
        jnp.concatenate([select, select], axis=1),
        jnp.concatenate([high, low], axis=1),
        NT,
    )


def lane_row(values):
    lane = iota((1, 128), 1)
    row = jnp.zeros((1, 128), F32)
    for index, value in enumerate(values):
        row = jnp.where(lane == index, value, row)
    return row


def push_select(z, row_meta):
    slots = z.slots * z.devices
    return (fiota((slots, 2 * z.lanes), 0) == row_meta[1:2, :]).astype(BF16)


def far_products(z, far_ref, col_meta, row_meta, source):
    onehot = (fiota((z.lanes, source.shape[0]), 1) == col_meta[:, 1:2]).astype(BF16)
    inputs = tile_inputs([(onehot, source)])
    products = tile_products(far_ref, z.half, inputs, z.lanes)
    return sum_rows(push_select(z, row_meta), products)


def prepare_kernel(
    z,
    rows_smem,
    rows_ref,
    cols_ref,
    defect_ref,
    coupling_ref,
    send_ref,
    far_ref,
    row_meta_ref,
    col_meta_ref,
    ids_ref,
    tiles,
    own,
    index,
    sems,
):
    me = lax.axis_index("blk")
    base = me * z.rows
    width = z.width
    near = jnp.int32(0)
    far = jnp.int32(0)
    for t in range(z.tiles):
        row = rows_smem[t]
        here = ((row >= base) & (row < base + z.rows)).astype(jnp.int32)
        ids_ref[near] = jnp.int32(t)
        ids_ref[z.half + 1 + far] = jnp.int32(t)
        near = near + here
        far = far + 1 - here
    copies = []
    for k in range(z.half):
        copy = pltpu.make_async_copy(
            coupling_ref.at[ids_ref[z.half + 1 + k]], tiles.at[k], sems.at[k]
        )
        copy.start()
        copies.append(copy)

    own[...] = jnp.zeros_like(own)
    own[0 : z.rows, :] = defect_ref[...]
    defect = own[...]

    count = index.shape[1]
    index[...] = jnp.full(index.shape, -1, jnp.int32)
    index[0:1, 0 : z.tiles] = rows_ref[...]
    index[1:2, 0 : z.tiles] = cols_ref[...]
    rows = index[0:1, :].astype(F32)
    cols = index[1:2, :].astype(F32)
    valid = rows >= 0
    row_owner = jnp.floor((rows + 0.5) * (1.0 / z.rows))
    col_owner = jnp.floor((cols + 0.5) * (1.0 / z.rows))
    row_local = rows - row_owner * z.rows
    col_local = cols - col_owner * z.rows
    mine = me.astype(F32)
    is_far = valid & (row_owner != mine)
    is_near = valid & (row_owner == mine)
    far_owner = jnp.where(is_far, row_owner, col_owner)
    far_local = jnp.where(is_far, row_local, col_local)
    own_local = jnp.where(is_far, col_local, row_local)
    kind = jnp.where(is_far, 1.0, jnp.where(is_near, 0.0, -1.0))
    key = jnp.where(valid, kind * z.devices + far_owner, -1.0)
    square = (count, count)
    before = iota(square, 0) < iota(square, 1)

    def ranks(value):
        wide = jnp.broadcast_to(value, square)
        same = (wide.T == wide) & before
        return jnp.sum(same.astype(F32), axis=0, keepdims=True)

    slot = ranks(key)
    position = ranks(kind)
    facts = jnp.concatenate(
        [
            far_owner,
            far_local,
            own_local + 1.0,
            slot * z.devices + far_owner + 1.0,
            slot,
            jnp.zeros((3, count), F32),
        ],
        axis=0,
    )
    facts = jnp.where(valid, facts, 0.0).astype(BF16)
    where = fiota((z.lanes, count), 0)
    near_pick = ((position == where) & is_near).astype(BF16)
    far_pick = ((position == where) & is_far).astype(BF16)
    near_rows = dot(facts, near_pick, NT)
    far_rows = dot(facts, far_pick, NT)
    near_cols = dot(near_pick, facts, NT)
    far_cols = dot(far_pick, facts, NT)

    place_row = fiota((1, z.lanes), 1) - z.half
    diag_row = (place_row >= 0) & (place_row < z.rows)
    near_target = jnp.where(diag_row, place_row, near_rows[2:3, :] - 1.0)
    far_target = far_rows[3:4, :] - 1.0
    row_meta_ref[...] = jnp.concatenate(
        [
            jnp.concatenate([near_target, near_target], axis=1),
            jnp.concatenate([far_target, far_target], axis=1),
            jnp.zeros((6, 2 * z.lanes), F32),
        ],
        axis=0,
    )
    lane = iota((z.lanes, 128), 1)
    place_col = fiota((z.lanes, 1), 0) - z.half
    diag_col = (place_col >= 0) & (place_col < z.rows)
    near_source = near_cols[:, 3:4] - 1.0
    first_source = near_cols[:, 0:1] * z.first_rows + near_cols[:, 1:2]
    first_source = jnp.where(near_source >= 0, first_source, -1.0)
    first_source = jnp.where(diag_col, mine * z.first_rows + place_col, first_source)
    near_source = jnp.where(diag_col, z.slots * z.devices + place_col, near_source)
    meta = jnp.where(lane == 0, near_source, 0.0)
    meta = jnp.where(lane == 1, far_cols[:, 2:3] - 1.0, meta)
    meta = jnp.where(lane == 2, first_source, meta)
    col_meta_ref[...] = meta

    owner = fiota((z.devices, z.lanes), 0)
    lane_f = lane.astype(F32)
    near_valid = near_cols[:, 3:4] > 0
    far_valid = far_cols[:, 3:4] > 0
    ask = jnp.where((lane_f == near_cols[:, 4:5]) & near_valid, near_cols[:, 1:2] + 1.0, 0.0)
    land = jnp.where(
        (lane_f == far_cols[:, 4:5] + z.slots) & far_valid, far_cols[:, 1:2] + 1.0, 0.0
    )
    info = dot(
        (owner == near_rows[0:1, :]).astype(BF16), ask.astype(BF16), NN
    ) + dot((owner == far_rows[0:1, :]).astype(BF16), land.astype(BF16), NN)

    send_ref[:, 0 : z.padded, :] = jnp.broadcast_to(
        defect[None, :, :], (z.devices, z.padded, width)
    )
    if z.first_rows > z.padded:
        send_ref[:, z.padded :, :] = jnp.zeros(
            (z.devices, z.first_rows - z.padded, width), F32
        )
    send_ref[:, z.info_row, :] = info

    onehot = (fiota((z.lanes, z.padded), 1) == (far_cols[:, 2:3] - 1.0)).astype(BF16)
    inputs = tile_inputs([(onehot, defect)])
    weights = jnp.concatenate([inputs, inputs], axis=1)
    acc = jnp.zeros((width, 2 * z.lanes), F32)
    for k in range(z.half):
        copies[k].wait()
        high, low = split(tiles[k])
        both = jnp.concatenate([high, low], axis=1)
        far_ref[k * width : (k + 1) * width, :] = both
        acc = place(dot(both, weights, NT), acc, k, z.lanes)
    pushes = sum_rows(push_select(z, row_meta_ref[...]), acc)
    for s in range(z.slots):
        send_ref[:, z.rows + s, :] = pushes[s * z.devices : (s + 1) * z.devices]


def gather_kernel(z, ids_ref, coupling_ref, diag_ref, near_ref, tiles, sems):
    width = z.width
    copies = []
    for k in range(z.near):
        source = coupling_ref.at[ids_ref[k]] if k < z.half else diag_ref.at[k - z.half]
        copy = pltpu.make_async_copy(source, tiles.at[k], sems.at[k])
        copy.start()
        copies.append(copy)
    for k in range(z.near):
        copies[k].wait()
        high, low = split(tiles[k])
        near_ref[k * width : (k + 1) * width, :] = jnp.concatenate([high, low], axis=1)


def own_rows(scratch, ref, z):
    scratch[...] = jnp.zeros_like(scratch)
    scratch[0 : z.rows, :] = ref[...]
    return scratch[...]


def landed(z, info, received):
    marks = []
    for s in range(z.slots):
        target = info[:, z.slots + s : z.slots + s + 1] - 1.0
        marks.append((fiota((z.devices, z.padded), 1) == target).astype(BF16))
    mark = jnp.concatenate(marks, axis=0)
    high, low = split(jnp.concatenate(received, axis=0))
    out = dot(mark, jnp.concatenate([high, low], axis=1), TN)
    return out[:, : z.width] + out[:, z.width :]


def fill_send(z, send_ref, info, far_ref, col_meta, row_meta, vector, dots):
    for s in range(z.slots):
        asked = info[:, s : s + 1] - 1.0
        onehot = (fiota((z.devices, z.padded), 1) == asked).astype(BF16)
        high, low = pick_rows(onehot, vector)
        send_ref[:, s, :] = high + low
    send_ref[:, 2 * z.slots, :] = jnp.broadcast_to(lane_row(dots), (z.devices, 128))
    pushes = far_products(z, far_ref, col_meta, row_meta, vector)
    for s in range(z.slots):
        send_ref[:, z.slots + s, :] = pushes[s * z.devices : (s + 1) * z.devices]


def near_select(z, row_meta):
    return (fiota((z.padded, 2 * z.lanes), 0) == row_meta[0:1, :]).astype(BF16)


def first_kernel(
    z,
    received_ref,
    near_ref,
    far_ref,
    defect_ref,
    mass_ref,
    row_meta_ref,
    col_meta_ref,
    send_ref,
    state_ref,
    info_ref,
    scalar_ref,
    own,
    own_mass,
):
    defect = own_rows(own, defect_ref, z)
    mass = own_rows(own_mass, mass_ref, z)
    row_meta = row_meta_ref[...]
    col_meta = col_meta_ref[...]
    everything = received_ref[...]
    real = iota(everything.shape, 1) < z.rows
    squares = jnp.sum(jnp.where(real, everything * everything, 0.0), axis=0)
    beta_square = total(squares)
    scale = -1.0 / jnp.sqrt(beta_square)
    flat = everything.reshape(z.devices * z.first_rows, z.width)
    onehot = (fiota((z.lanes, flat.shape[0]), 1) == col_meta[:, 2:3]).astype(BF16)
    inputs = tile_inputs([(onehot, flat)])
    products = tile_products(near_ref, z.near, inputs, z.lanes)
    image = mass * defect + sum_rows(near_select(z, row_meta), products)
    info = received_ref[:, z.info_row, :]
    info_ref[...] = info
    image = image + landed(
        z, info, [received_ref[:, z.rows + s, :] for s in range(z.slots)]
    )
    v0 = defect * scale
    w0 = image * scale
    dots = [total(w0 * v0), total(w0 * w0)]
    state_ref[0] = v0
    state_ref[1] = w0
    scalar_ref[...] = jnp.broadcast_to(jnp.sqrt(beta_square), scalar_ref.shape)
    fill_send(z, send_ref, info, far_ref, col_meta, row_meta, w0, dots)


def apply_received(z, received_ref, near_ref, info, mass, row_meta, col_meta, vector):
    sources = [received_ref[:, s, :] for s in range(z.slots)] + [vector]
    source = jnp.concatenate(sources, axis=0)
    onehot = (fiota((z.lanes, source.shape[0]), 1) == col_meta[:, 0:1]).astype(BF16)
    inputs = tile_inputs([(onehot, source)])
    products = tile_products(near_ref, z.near, inputs, z.lanes)
    image = mass * vector + sum_rows(near_select(z, row_meta), products)
    return image + landed(
        z, info, [received_ref[:, z.slots + s, :] for s in range(z.slots)]
    )


def summed_dots(z, received_ref, row):
    sums = jnp.sum(received_ref[:, row, :], axis=0, keepdims=True)
    return lambda index: sums[:, index : index + 1]


def second_kernel(
    z,
    received_ref,
    near_ref,
    far_ref,
    mass_ref,
    row_meta_ref,
    col_meta_ref,
    state_in,
    info_ref,
    scalar_in,
    send_ref,
    state_ref,
    scalar_ref,
    own_mass,
):
    mass = own_rows(own_mass, mass_ref, z)
    row_meta = row_meta_ref[...]
    col_meta = col_meta_ref[...]
    info = info_ref[...]
    v0 = state_in[0]
    w0 = state_in[1]
    image = apply_received(
        z, received_ref, near_ref, info, mass, row_meta, col_meta, w0
    )
    get = summed_dots(z, received_ref, 2 * z.slots)
    h00, g00 = get(0), get(1)
    inverse = lax.rsqrt(jnp.maximum(g00 - h00 * h00, FLOOR * g00))
    v1 = (w0 - h00 * v0) * inverse
    w1 = (image - h00 * w0) * inverse
    dots = [total(w1 * v0), total(w1 * v1), total(w1 * w1), total(w1 * w0)]
    state_ref[0] = v0
    state_ref[1] = v1
    state_ref[2] = w0
    state_ref[3] = w1
    scalar_ref[...] = jnp.broadcast_to(
        lane_row([scalar_in[0:1, 0:1], h00, g00]), scalar_ref.shape
    )
    fill_send(z, send_ref, info, far_ref, col_meta, row_meta, w1, dots)


def third_kernel(
    z,
    received_ref,
    near_ref,
    mass_ref,
    row_meta_ref,
    col_meta_ref,
    state_in,
    info_ref,
    scalar_in,
    send_ref,
    state_ref,
    scalar_ref,
    own_mass,
):
    mass = own_rows(own_mass, mass_ref, z)
    v0, v1, w0, w1 = state_in[0], state_in[1], state_in[2], state_in[3]
    image = apply_received(
        z,
        received_ref,
        near_ref,
        info_ref[...],
        mass,
        row_meta_ref[...],
        col_meta_ref[...],
        w1,
    )
    get = summed_dots(z, received_ref, 2 * z.slots)
    h01, h11, g11, g01 = get(0), get(1), get(2), get(3)
    inverse = lax.rsqrt(jnp.maximum(g11 - h01 * h01 - h11 * h11, FLOOR * g11))
    v2 = (w1 - h01 * v0 - h11 * v1) * inverse
    w2 = (image - h01 * w0 - h11 * w1) * inverse
    dots = [total(w2 * v0), total(w2 * w0), total(w2 * w1), total(w2 * w2)]
    state_ref[0] = v0
    state_ref[1] = v1
    state_ref[2] = v2
    old = scalar_in[0:1, :]
    scalar_ref[...] = jnp.broadcast_to(
        lane_row([old[:, 0:1], old[:, 1:2], old[:, 2:3], h01, g01, g11]),
        scalar_ref.shape,
    )
    send_ref[:, 0, :] = jnp.broadcast_to(lane_row(dots), (z.devices, 128))


def last_kernel(z, received_ref, state_in, scalar_in, out_ref):
    get = summed_dots(z, received_ref, 0)
    d, g02, g12, g22 = get(0), get(1), get(2), get(3)
    old = scalar_in[0:1, :]
    beta, h00, g00 = old[:, 0:1], old[:, 1:2], old[:, 2:3]
    h01, g01, g11 = old[:, 3:4], old[:, 4:5], old[:, 5:6]
    b0, b1, b2 = beta * h00, beta * h01, beta * d
    l00 = jnp.sqrt(g00)
    l10 = g01 / l00
    l20 = g02 / l00
    l11 = jnp.sqrt(g11 - l10 * l10)
    l21 = (g12 - l20 * l10) / l11
    l22 = jnp.sqrt(g22 - l20 * l20 - l21 * l21)
    f0 = b0 / l00
    f1 = (b1 - l10 * f0) / l11
    f2 = (b2 - l20 * f0 - l21 * f1) / l22
    y2 = f2 / l22
    y1 = (f1 - l21 * y2) / l11
    y0 = (f0 - l10 * y1 - l20 * y2) / l00
    update = y0 * state_in[0] + y1 * state_in[1] + y2 * state_in[2]
    out_ref[...] = update[0 : z.rows, :]


def on_device(defect, mass, block_diag, coupling, tile_rows, tile_cols):
    z = Sizes(lax.axis_size("blk"), defect.shape[0], defect.shape[1], tile_rows.shape[0])
    width = z.width
    vmem = pl.BlockSpec(memory_space=pltpu.VMEM)
    smem = pl.BlockSpec(memory_space=pltpu.SMEM)
    anywhere = pl.BlockSpec(memory_space=pl.ANY)

    def shape(*dims, dtype=F32):
        return jax.ShapeDtypeStruct(dims, dtype)

    def call(kernel, name, ins, outs, scratch, args, limit):
        return pl.pallas_call(
            functools.partial(kernel, z),
            out_shape=[item[0] for item in outs],
            in_specs=ins,
            out_specs=[item[1] for item in outs],
            scratch_shapes=scratch,
            name=name,
            compiler_params=pltpu.CompilerParams(vmem_limit_bytes=limit * MIB),
        )(*args)

    rows_2d = tile_rows.reshape(1, z.tiles)
    cols_2d = tile_cols.reshape(1, z.tiles)
    index_width = round_up(z.tiles, 128)
    tile_bytes = -(-z.near * width * width * 4 // MIB)
    send, far, row_meta, col_meta, ids = call(
        prepare_kernel,
        "prepare",
        [smem, vmem, vmem, vmem, anywhere],
        [
            (shape(z.devices, z.first_rows, width), vmem),
            (shape(z.half * width, 2 * width, dtype=BF16), vmem),
            (shape(8, 2 * z.lanes), vmem),
            (shape(z.lanes, 128), vmem),
            (shape(2 * z.half + 2, dtype=jnp.int32), smem),
        ],
        [
            pltpu.VMEM((z.half, width, width), F32),
            pltpu.VMEM((z.padded, width), F32),
            pltpu.VMEM((8, index_width), jnp.int32),
            pltpu.SemaphoreType.DMA((z.half,)),
        ],
        (tile_rows, rows_2d, cols_2d, defect, coupling),
        2 * tile_bytes + 8,
    )
    received = lax.all_to_all(send, "blk", split_axis=0, concat_axis=0, tiled=True)
    (near,) = call(
        gather_kernel,
        "gather",
        [smem, anywhere, anywhere],
        [(shape(z.near * width, 2 * width, dtype=BF16), vmem)],
        [
            pltpu.VMEM((z.near, width, width), F32),
            pltpu.SemaphoreType.DMA((z.near,)),
        ],
        (ids, coupling, block_diag),
        2 * tile_bytes + 4,
    )
    send, state, info, scalars = call(
        first_kernel,
        "first",
        [vmem] * 7,
        [
            (shape(z.devices, z.send_rows, width), vmem),
            (shape(2, z.padded, width), vmem),
            (shape(z.devices, 128), vmem),
            (shape(8, 128), vmem),
        ],
        [pltpu.VMEM((z.padded, width), F32)] * 2,
        (received, near, far, defect, mass, row_meta, col_meta),
        2 * tile_bytes + 8,
    )
    received = lax.all_to_all(send, "blk", split_axis=0, concat_axis=0, tiled=True)
    send, state, scalars = call(
        second_kernel,
        "second",
        [vmem] * 9,
        [
            (shape(z.devices, z.send_rows, width), vmem),
            (shape(4, z.padded, width), vmem),
            (shape(8, 128), vmem),
        ],
        [pltpu.VMEM((z.padded, width), F32)],
        (received, near, far, mass, row_meta, col_meta, state, info, scalars),
        2 * tile_bytes + 8,
    )
    received = lax.all_to_all(send, "blk", split_axis=0, concat_axis=0, tiled=True)
    send, state, scalars = call(
        third_kernel,
        "third",
        [vmem] * 8,
        [
            (shape(z.devices, 1, width), vmem),
            (shape(3, z.padded, width), vmem),
            (shape(8, 128), vmem),
        ],
        [pltpu.VMEM((z.padded, width), F32)],
        (received, near, mass, row_meta, col_meta, state, info, scalars),
        2 * tile_bytes + 8,
    )
    received = lax.all_to_all(send, "blk", split_axis=0, concat_axis=0, tiled=True)
    (update,) = call(
        last_kernel,
        "last",
        [vmem] * 3,
        [(shape(z.rows, width), vmem)],
        [],
        (received, state, scalars),
        4,
    )
    return update


def solution(mesh):
    in_specs = (
        P("blk", None),
        P("blk", None),
        P("blk", None, None),
        P("blk", None, None),
        P("blk"),
        P("blk"),
    )
    return jax.shard_map(
        on_device, mesh=mesh, in_specs=in_specs, out_specs=P("blk", None), check_vma=False
    )
```

```python
import functools

import jax
import jax.numpy as jnp
from jax import lax
from jax.experimental import pallas as pl
from jax.experimental.pallas import tpu as pltpu
from jax.sharding import PartitionSpec as P

F32 = jnp.float32
BF16 = jnp.bfloat16
NT = (((1,), (1,)), ((), ()))
NN = (((1,), (0,)), ((), ()))
TN = (((0,), (0,)), ((), ()))
FLOOR = 2.0**-22
MIB = 1 << 20
GROUP = 12


def round_up(value, step):
    return -(-value // step) * step


class Sizes:
    def __init__(self, devices, rows, width, tiles):
        self.devices = devices
        self.rows = rows
        self.width = width
        self.tiles = tiles
        self.half = tiles // 2
        self.slots = (self.half + devices - 2) // (devices - 1)
        self.padded = round_up(rows, 8)
        self.near = self.half + rows
        self.lanes = round_up(self.near, 64)
        self.first_rows = round_up(rows + self.slots + 1, 8)
        self.info_row = rows + self.slots
        self.send_rows = 2 * self.slots + 1


def dot(a, b, dims):
    return lax.dot_general(a, b, dims, preferred_element_type=F32)


def split(value):
    high = value.astype(BF16)
    low = (value - high.astype(F32)).astype(BF16)
    return high, low


def iota(shape, axis):
    return lax.broadcasted_iota(jnp.int32, shape, axis)


def fiota(shape, axis):
    return iota(shape, axis).astype(F32)


def total(value):
    return jnp.sum(jnp.sum(value, axis=0, keepdims=True), axis=1, keepdims=True)


def pick_rows(onehot, source):
    width = source.shape[1]
    high, low = split(source)
    out = dot(onehot, jnp.concatenate([high, low], axis=1), NN)
    return out[:, :width], out[:, width:]


def tile_inputs(pairs):
    high = low = None
    for onehot, source in pairs:
        h, l = pick_rows(onehot, source)
        high = h if high is None else high + h
        low = l if low is None else low + l
    return jnp.concatenate([high, low], axis=0).astype(BF16)


def place(result, acc, index, lanes):
    lane = iota(acc.shape, 1)
    return jnp.where((lane == index) | (lane == lanes + index), result, acc)


def tile_products(tiles_ref, count, inputs, lanes, group=4):
    width = inputs.shape[1]
    weights = jnp.concatenate([inputs, inputs], axis=1)
    acc = jnp.zeros((width, 2 * lanes), F32)
    for start in range(0, count, group):
        size = min(group, count - start)
        out = dot(tiles_ref[start * width : (start + size) * width, :], weights, NT)
        for inner in range(size):
            acc = place(out[inner * width : (inner + 1) * width], acc, start + inner, lanes)
    return acc


def sum_rows(select, products):
    high, low = split(products)
    return dot(
        jnp.concatenate([select, select], axis=1),
        jnp.concatenate([high, low], axis=1),
        NT,
    )


def lane_row(values):
    lane = iota((1, 128), 1)
    row = jnp.zeros((1, 128), F32)
    for index, value in enumerate(values):
        row = jnp.where(lane == index, value, row)
    return row


def push_select(z, row_meta):
    slots = z.slots * z.devices
    return (fiota((slots, 2 * z.lanes), 0) == row_meta[1:2, :]).astype(BF16)


def far_products(z, far_ref, col_meta, row_meta, source):
    onehot = (fiota((z.lanes, source.shape[0]), 1) == col_meta[:, 1:2]).astype(BF16)
    inputs = tile_inputs([(onehot, source)])
    products = tile_products(far_ref, z.half, inputs, z.lanes)
    return sum_rows(push_select(z, row_meta), products)


def prepare_kernel(
    z,
    rows_hbm,
    rows_2d_hbm,
    cols_2d_hbm,
    defect_hbm,
    coupling_hbm,
    send_ref,
    far_ref,
    row_meta_ref,
    col_meta_ref,
    ids_ref,
    rows_smem,
    rows_ref,
    cols_ref,
    defect_ref,
    tiles,
    own,
    index,
    small_sems,
    sems,
):
    me = lax.axis_index("blk")
    base = me * z.rows
    width = z.width
    small = [
        pltpu.make_async_copy(source, target, small_sems.at[i])
        for i, (source, target) in enumerate(
            [
                (rows_hbm, rows_smem),
                (rows_2d_hbm, rows_ref),
                (cols_2d_hbm, cols_ref),
                (defect_hbm, defect_ref),
            ]
        )
    ]
    for copy in small:
        copy.start()
    own[...] = jnp.zeros_like(own)
    index[...] = jnp.full(index.shape, -1, jnp.int32)
    small[0].wait()
    near = jnp.int32(0)
    far = jnp.int32(0)
    for t in range(z.tiles):
        row = rows_smem[t]
        here = ((row >= base) & (row < base + z.rows)).astype(jnp.int32)
        ids_ref[near] = jnp.int32(t)
        ids_ref[z.half + 1 + far] = jnp.int32(t)
        near = near + here
        far = far + 1 - here
    copies = []
    for k in range(z.half):
        copy = pltpu.make_async_copy(
            coupling_hbm.at[ids_ref[z.half + 1 + k]], tiles.at[k], sems.at[k]
        )
        copy.start()
        copies.append(copy)
    for copy in small[1:]:
        copy.wait()

    own[0 : z.rows, :] = defect_ref[...]
    defect = own[...]

    count = index.shape[1]
    index[0:1, 0 : z.tiles] = rows_ref[...]
    index[1:2, 0 : z.tiles] = cols_ref[...]
    rows = index[0:1, :].astype(F32)
    cols = index[1:2, :].astype(F32)
    valid = rows >= 0
    row_owner = jnp.floor((rows + 0.5) * (1.0 / z.rows))
    col_owner = jnp.floor((cols + 0.5) * (1.0 / z.rows))
    row_local = rows - row_owner * z.rows
    col_local = cols - col_owner * z.rows
    mine = me.astype(F32)
    is_far = valid & (row_owner != mine)
    is_near = valid & (row_owner == mine)
    far_owner = jnp.where(is_far, row_owner, col_owner)
    far_local = jnp.where(is_far, row_local, col_local)
    own_local = jnp.where(is_far, col_local, row_local)
    kind = jnp.where(is_far, 1.0, jnp.where(is_near, 0.0, -1.0))
    key = jnp.where(valid, kind * z.devices + far_owner, -1.0)
    square = (count, count)
    before = iota(square, 0) < iota(square, 1)

    def ranks(value):
        wide = jnp.broadcast_to(value, square)
        same = (wide.T == wide) & before
        return jnp.sum(same.astype(F32), axis=0, keepdims=True)

    slot = ranks(key)
    position = ranks(kind)
    facts = jnp.concatenate(
        [
            far_owner,
            far_local,
            own_local + 1.0,
            slot * z.devices + far_owner + 1.0,
            slot,
            jnp.zeros((3, count), F32),
        ],
        axis=0,
    )
    facts = jnp.where(valid, facts, 0.0).astype(BF16)
    where = fiota((z.lanes, count), 0)
    near_pick = ((position == where) & is_near).astype(BF16)
    far_pick = ((position == where) & is_far).astype(BF16)
    near_rows = dot(facts, near_pick, NT)
    far_rows = dot(facts, far_pick, NT)
    near_cols = dot(near_pick, facts, NT)
    far_cols = dot(far_pick, facts, NT)

    place_row = fiota((1, z.lanes), 1) - z.half
    diag_row = (place_row >= 0) & (place_row < z.rows)
    near_target = jnp.where(diag_row, place_row, near_rows[2:3, :] - 1.0)
    far_target = far_rows[3:4, :] - 1.0
    row_meta = jnp.concatenate(
        [
            jnp.concatenate([near_target, near_target], axis=1),
            jnp.concatenate([far_target, far_target], axis=1),
            jnp.zeros((6, 2 * z.lanes), F32),
        ],
        axis=0,
    )
    row_meta_ref[...] = row_meta
    lane = iota((z.lanes, 128), 1)
    place_col = fiota((z.lanes, 1), 0) - z.half
    diag_col = (place_col >= 0) & (place_col < z.rows)
    near_source = near_cols[:, 3:4] - 1.0
    first_source = near_cols[:, 0:1] * z.first_rows + near_cols[:, 1:2]
    first_source = jnp.where(near_source >= 0, first_source, -1.0)
    first_source = jnp.where(diag_col, mine * z.first_rows + place_col, first_source)
    near_source = jnp.where(diag_col, z.slots * z.devices + place_col, near_source)
    meta = jnp.where(lane == 0, near_source, 0.0)
    meta = jnp.where(lane == 1, far_cols[:, 2:3] - 1.0, meta)
    meta = jnp.where(lane == 2, first_source, meta)
    col_meta_ref[...] = meta

    owner = fiota((z.devices, z.lanes), 0)
    lane_f = lane.astype(F32)
    near_valid = near_cols[:, 3:4] > 0
    far_valid = far_cols[:, 3:4] > 0
    ask = jnp.where((lane_f == near_cols[:, 4:5]) & near_valid, near_cols[:, 1:2] + 1.0, 0.0)
    land = jnp.where(
        (lane_f == far_cols[:, 4:5] + z.slots) & far_valid, far_cols[:, 1:2] + 1.0, 0.0
    )
    info = dot(
        (owner == near_rows[0:1, :]).astype(BF16), ask.astype(BF16), NN
    ) + dot((owner == far_rows[0:1, :]).astype(BF16), land.astype(BF16), NN)

    send_ref[:, 0 : z.padded, :] = jnp.broadcast_to(
        defect[None, :, :], (z.devices, z.padded, width)
    )
    if z.first_rows > z.padded:
        send_ref[:, z.padded :, :] = jnp.zeros(
            (z.devices, z.first_rows - z.padded, width), F32
        )
    send_ref[:, z.info_row, :] = info

    onehot = (fiota((z.lanes, z.padded), 1) == (far_cols[:, 2:3] - 1.0)).astype(BF16)
    inputs = tile_inputs([(onehot, defect)])
    weights = jnp.concatenate([inputs, inputs], axis=1)
    acc = jnp.zeros((width, 2 * z.lanes), F32)
    for start in range(0, z.half, GROUP):
        group = range(start, min(start + GROUP, z.half))
        for k in group:
            copies[k].wait()
        for k in group:
            far_ref[k * width : (k + 1) * width, :] = both_pieces(tiles[k])
        out = dot(
            far_ref[start * width : (group[-1] + 1) * width, :], weights, NT
        )
        for k in group:
            acc = place(out[(k - start) * width : (k - start + 1) * width], acc, k, z.lanes)
    pushes = sum_rows(push_select(z, row_meta), acc)
    for s in range(z.slots):
        send_ref[:, z.rows + s, :] = pushes[s * z.devices : (s + 1) * z.devices]


def both_pieces(tile):
    high, low = split(tile)
    return jnp.concatenate([high, low], axis=1)


def own_rows(scratch, ref, z):
    scratch[...] = jnp.zeros_like(scratch)
    scratch[0 : z.rows, :] = ref[...]
    return scratch[...]


def landed(z, info, received):
    marks = []
    for s in range(z.slots):
        target = info[:, z.slots + s : z.slots + s + 1] - 1.0
        marks.append((fiota((z.devices, z.padded), 1) == target).astype(BF16))
    mark = jnp.concatenate(marks, axis=0)
    high, low = split(jnp.concatenate(received, axis=0))
    out = dot(mark, jnp.concatenate([high, low], axis=1), TN)
    return out[:, : z.width] + out[:, z.width :]


def fill_send(z, send_ref, info, far_ref, col_meta, row_meta, vector, dots):
    for s in range(z.slots):
        asked = info[:, s : s + 1] - 1.0
        onehot = (fiota((z.devices, z.padded), 1) == asked).astype(BF16)
        high, low = pick_rows(onehot, vector)
        send_ref[:, s, :] = high + low
    send_ref[:, 2 * z.slots, :] = jnp.broadcast_to(lane_row(dots), (z.devices, 128))
    pushes = far_products(z, far_ref, col_meta, row_meta, vector)
    for s in range(z.slots):
        send_ref[:, z.slots + s, :] = pushes[s * z.devices : (s + 1) * z.devices]


def near_select(z, row_meta):
    return (fiota((z.padded, 2 * z.lanes), 0) == row_meta[0:1, :]).astype(BF16)


def first_kernel(
    z,
    received_ref,
    far_ref,
    row_meta_ref,
    col_meta_ref,
    ids_hbm,
    defect_hbm,
    mass_hbm,
    coupling_hbm,
    diag_hbm,
    send_ref,
    state_ref,
    info_ref,
    scalar_ref,
    near_ref,
    mass_out_ref,
    ids_ref,
    defect_ref,
    mass_ref,
    tiles,
    diag,
    own,
    own_mass,
    small_sems,
    sems,
):
    width = z.width
    ids_copy = pltpu.make_async_copy(ids_hbm, ids_ref, small_sems.at[0])
    diag_copy = pltpu.make_async_copy(diag_hbm, diag, small_sems.at[1])
    defect_copy = pltpu.make_async_copy(defect_hbm, defect_ref, small_sems.at[2])
    mass_copy = pltpu.make_async_copy(mass_hbm, mass_ref, small_sems.at[3])
    for copy in (ids_copy, defect_copy, mass_copy, diag_copy):
        copy.start()
    ids_copy.wait()
    copies = []
    for k in range(z.half):
        copy = pltpu.make_async_copy(
            coupling_hbm.at[ids_ref[k]], tiles.at[k], sems.at[k]
        )
        copy.start()
        copies.append(copy)
    defect_copy.wait()
    mass_copy.wait()
    defect = own_rows(own, defect_ref, z)
    mass = own_rows(own_mass, mass_ref, z)
    row_meta = row_meta_ref[...]
    col_meta = col_meta_ref[...]
    everything = received_ref[...]
    real = iota(everything.shape, 1) < z.rows
    squares = jnp.sum(jnp.where(real, everything * everything, 0.0), axis=0)
    beta_square = total(squares)
    scale = -1.0 / jnp.sqrt(beta_square)
    flat = everything.reshape(z.devices * z.first_rows, z.width)
    onehot = (fiota((z.lanes, flat.shape[0]), 1) == col_meta[:, 2:3]).astype(BF16)
    inputs = tile_inputs([(onehot, flat)])
    weights = jnp.concatenate([inputs, inputs], axis=1)
    products = jnp.zeros((width, 2 * z.lanes), F32)
    diag_copy.wait()
    groups = [range(z.half, z.near)]
    groups += [
        range(start, min(start + GROUP, z.half)) for start in range(0, z.half, GROUP)
    ]
    for group in groups:
        if group[0] < z.half:
            for k in group:
                copies[k].wait()
        for k in group:
            tile = tiles[k] if k < z.half else diag[k - z.half]
            near_ref[k * width : (k + 1) * width, :] = both_pieces(tile)
        low, high = group[0] * width, (group[-1] + 1) * width
        out = dot(near_ref[low:high, :], weights, NT)
        for i, k in enumerate(group):
            products = place(out[i * width : (i + 1) * width], products, k, z.lanes)
    image = mass * defect + sum_rows(near_select(z, row_meta), products)
    info = received_ref[:, z.info_row, :]
    info_ref[...] = info
    image = image + landed(
        z, info, [received_ref[:, z.rows + s, :] for s in range(z.slots)]
    )
    v0 = defect * scale
    w0 = image * scale
    dots = [total(w0 * v0), total(w0 * w0)]
    state_ref[0] = v0
    state_ref[1] = w0
    mass_out_ref[...] = mass
    scalar_ref[...] = jnp.broadcast_to(jnp.sqrt(beta_square), scalar_ref.shape)
    fill_send(z, send_ref, info, far_ref, col_meta, row_meta, w0, dots)


def apply_received(z, received_ref, near_ref, info, mass, row_meta, col_meta, vector):
    sources = [received_ref[:, s, :] for s in range(z.slots)] + [vector]
    source = jnp.concatenate(sources, axis=0)
    onehot = (fiota((z.lanes, source.shape[0]), 1) == col_meta[:, 0:1]).astype(BF16)
    inputs = tile_inputs([(onehot, source)])
    products = tile_products(near_ref, z.near, inputs, z.lanes)
    image = mass * vector + sum_rows(near_select(z, row_meta), products)
    return image + landed(
        z, info, [received_ref[:, z.slots + s, :] for s in range(z.slots)]
    )


def summed_dots(z, received_ref, row):
    sums = jnp.sum(received_ref[:, row, :], axis=0, keepdims=True)
    return lambda index: sums[:, index : index + 1]


def second_kernel(
    z,
    received_ref,
    near_ref,
    far_ref,
    mass_ref,
    row_meta_ref,
    col_meta_ref,
    state_in,
    info_ref,
    scalar_in,
    send_ref,
    state_ref,
    scalar_ref,
):
    mass = mass_ref[...]
    row_meta = row_meta_ref[...]
    col_meta = col_meta_ref[...]
    info = info_ref[...]
    v0 = state_in[0]
    w0 = state_in[1]
    image = apply_received(
        z, received_ref, near_ref, info, mass, row_meta, col_meta, w0
    )
    get = summed_dots(z, received_ref, 2 * z.slots)
    h00, g00 = get(0), get(1)
    inverse = lax.rsqrt(jnp.maximum(g00 - h00 * h00, FLOOR * g00))
    v1 = (w0 - h00 * v0) * inverse
    w1 = (image - h00 * w0) * inverse
    dots = [total(w1 * v0), total(w1 * v1), total(w1 * w1), total(w1 * w0)]
    state_ref[0] = v0
    state_ref[1] = v1
    state_ref[2] = w0
    state_ref[3] = w1
    scalar_ref[...] = jnp.broadcast_to(
        lane_row([scalar_in[0:1, 0:1], h00, g00]), scalar_ref.shape
    )
    fill_send(z, send_ref, info, far_ref, col_meta, row_meta, w1, dots)


def third_kernel(
    z,
    received_ref,
    near_ref,
    mass_ref,
    row_meta_ref,
    col_meta_ref,
    state_in,
    info_ref,
    scalar_in,
    send_ref,
    state_ref,
    scalar_ref,
):
    mass = mass_ref[...]
    v0, v1, w0, w1 = state_in[0], state_in[1], state_in[2], state_in[3]
    image = apply_received(
        z,
        received_ref,
        near_ref,
        info_ref[...],
        mass,
        row_meta_ref[...],
        col_meta_ref[...],
        w1,
    )
    get = summed_dots(z, received_ref, 2 * z.slots)
    h01, h11, g11, g01 = get(0), get(1), get(2), get(3)
    inverse = lax.rsqrt(jnp.maximum(g11 - h01 * h01 - h11 * h11, FLOOR * g11))
    v2 = (w1 - h01 * v0 - h11 * v1) * inverse
    w2 = (image - h01 * w0 - h11 * w1) * inverse
    dots = [total(w2 * v0), total(w2 * w0), total(w2 * w1), total(w2 * w2)]
    state_ref[0] = v0
    state_ref[1] = v1
    state_ref[2] = v2
    old = scalar_in[0:1, :]
    scalar_ref[...] = jnp.broadcast_to(
        lane_row([old[:, 0:1], old[:, 1:2], old[:, 2:3], h01, g01, g11]),
        scalar_ref.shape,
    )
    send_ref[:, 0, :] = jnp.broadcast_to(lane_row(dots), (z.devices, 128))


def last_kernel(z, received_ref, state_in, scalar_in, out_ref):
    get = summed_dots(z, received_ref, 0)
    d, g02, g12, g22 = get(0), get(1), get(2), get(3)
    old = scalar_in[0:1, :]
    beta, h00, g00 = old[:, 0:1], old[:, 1:2], old[:, 2:3]
    h01, g01, g11 = old[:, 3:4], old[:, 4:5], old[:, 5:6]
    b0, b1, b2 = beta * h00, beta * h01, beta * d
    l00 = jnp.sqrt(g00)
    l10 = g01 / l00
    l20 = g02 / l00
    l11 = jnp.sqrt(g11 - l10 * l10)
    l21 = (g12 - l20 * l10) / l11
    l22 = jnp.sqrt(g22 - l20 * l20 - l21 * l21)
    f0 = b0 / l00
    f1 = (b1 - l10 * f0) / l11
    f2 = (b2 - l20 * f0 - l21 * f1) / l22
    y2 = f2 / l22
    y1 = (f1 - l21 * y2) / l11
    y0 = (f0 - l10 * y1 - l20 * y2) / l00
    update = y0 * state_in[0] + y1 * state_in[1] + y2 * state_in[2]
    out_ref[...] = update[0 : z.rows, :]


def on_device(defect, mass, block_diag, coupling, tile_rows, tile_cols):
    z = Sizes(lax.axis_size("blk"), defect.shape[0], defect.shape[1], tile_rows.shape[0])
    width = z.width
    vmem = pl.BlockSpec(memory_space=pltpu.VMEM)
    smem = pl.BlockSpec(memory_space=pltpu.SMEM)
    hbm = pl.BlockSpec(memory_space=pltpu.HBM)

    def shape(*dims, dtype=F32):
        return jax.ShapeDtypeStruct(dims, dtype)

    def call(kernel, name, ins, outs, scratch, args, limit):
        return pl.pallas_call(
            functools.partial(kernel, z),
            out_shape=[item[0] for item in outs],
            in_specs=ins,
            out_specs=[item[1] for item in outs],
            scratch_shapes=scratch,
            name=name,
            compiler_params=pltpu.CompilerParams(vmem_limit_bytes=limit * MIB),
        )(*args)

    def in_hbm(value):
        return pltpu.with_memory_space_constraint(value, pltpu.HBM)

    rows_2d = in_hbm(tile_rows.reshape(1, z.tiles))
    cols_2d = in_hbm(tile_cols.reshape(1, z.tiles))
    tile_rows, coupling, block_diag, defect, mass = map(
        in_hbm, (tile_rows, coupling, block_diag, defect, mass)
    )
    index_width = round_up(z.tiles, 128)
    tile = width * width * 4
    send, far, row_meta, col_meta, ids = call(
        prepare_kernel,
        "prepare",
        [hbm] * 5,
        [
            (shape(z.devices, z.first_rows, width), vmem),
            (shape(z.half * width, 2 * width, dtype=BF16), vmem),
            (shape(8, 2 * z.lanes), vmem),
            (shape(z.lanes, 128), vmem),
            (shape(2 * z.half + 2, dtype=jnp.int32), smem),
        ],
        [
            pltpu.SMEM((z.tiles,), jnp.int32),
            pltpu.VMEM((1, z.tiles), jnp.int32),
            pltpu.VMEM((1, z.tiles), jnp.int32),
            pltpu.VMEM((z.rows, width), F32),
            pltpu.VMEM((z.half, width, width), F32),
            pltpu.VMEM((z.padded, width), F32),
            pltpu.VMEM((8, index_width), jnp.int32),
            pltpu.SemaphoreType.DMA((4,)),
            pltpu.SemaphoreType.DMA((z.half,)),
        ],
        (tile_rows, rows_2d, cols_2d, defect, coupling),
        2 * z.half * tile // MIB + 4,
    )
    received = lax.all_to_all(send, "blk", split_axis=0, concat_axis=0, tiled=True)
    send, state, info, scalars, near, mass = call(
        first_kernel,
        "first",
        [vmem] * 4 + [hbm] * 5,
        [
            (shape(z.devices, z.send_rows, width), vmem),
            (shape(2, z.padded, width), vmem),
            (shape(z.devices, 128), vmem),
            (shape(8, 128), vmem),
            (shape(z.near * width, 2 * width, dtype=BF16), vmem),
            (shape(z.padded, width), vmem),
        ],
        [
            pltpu.SMEM((2 * z.half + 2,), jnp.int32),
            pltpu.VMEM((z.rows, width), F32),
            pltpu.VMEM((z.rows, width), F32),
            pltpu.VMEM((z.half, width, width), F32),
            pltpu.VMEM((z.rows, width, width), F32),
            pltpu.VMEM((z.padded, width), F32),
            pltpu.VMEM((z.padded, width), F32),
            pltpu.SemaphoreType.DMA((4,)),
            pltpu.SemaphoreType.DMA((z.half,)),
        ],
        (received, far, row_meta, col_meta, ids, defect, mass, coupling, block_diag),
        2 * z.near * tile // MIB + 4,
    )
    received = lax.all_to_all(send, "blk", split_axis=0, concat_axis=0, tiled=True)
    send, state, scalars = call(
        second_kernel,
        "second",
        [vmem] * 9,
        [
            (shape(z.devices, z.send_rows, width), vmem),
            (shape(4, z.padded, width), vmem),
            (shape(8, 128), vmem),
        ],
        [],
        (received, near, far, mass, row_meta, col_meta, state, info, scalars),
        4,
    )
    received = lax.all_to_all(send, "blk", split_axis=0, concat_axis=0, tiled=True)
    send, state, scalars = call(
        third_kernel,
        "third",
        [vmem] * 8,
        [
            (shape(z.devices, 1, width), vmem),
            (shape(3, z.padded, width), vmem),
            (shape(8, 128), vmem),
        ],
        [],
        (received, near, mass, row_meta, col_meta, state, info, scalars),
        4,
    )
    received = lax.all_to_all(send, "blk", split_axis=0, concat_axis=0, tiled=True)
    (update,) = call(
        last_kernel,
        "last",
        [vmem] * 3,
        [(shape(z.rows, width), vmem)],
        [],
        (received, state, scalars),
        4,
    )
    return update


def solution(mesh):
    in_specs = (
        P("blk", None),
        P("blk", None),
        P("blk", None, None),
        P("blk", None, None),
        P("blk"),
        P("blk"),
    )
    return jax.shard_map(
        on_device, mesh=mesh, in_specs=in_specs, out_specs=P("blk", None), check_vma=False
    )
```

```python
import functools

import jax
import jax.numpy as jnp
from jax import lax
from jax.experimental import pallas as pl
from jax.experimental.pallas import tpu as pltpu
from jax.sharding import PartitionSpec as P

F32 = jnp.float32
BF16 = jnp.bfloat16
NT = (((1,), (1,)), ((), ()))
NN = (((1,), (0,)), ((), ()))
FLOOR = 2.0**-22
MIB = 1 << 20
CHUNK = 32
OCTET = 8


def round_up(value, step):
    return -(-value // step) * step


class Sizes:
    def __init__(self, devices, rows, width, tiles):
        self.devices = devices
        self.rows = rows
        self.width = width
        self.tiles = tiles
        self.half = tiles // 2
        self.near = self.half + rows
        self.slots = (self.half + devices - 2) // (devices - 1)
        self.cells = self.slots * devices
        self.padded = round_up(rows, 16)
        self.near_rows = 2 * round_up(self.near, OCTET)
        self.far_rows = 2 * round_up(self.half, OCTET)
        self.first_rows = rows + self.slots + 1
        self.info_row = rows + self.slots
        self.send_rows = 2 * self.slots + 1
        self.dots_row = 2 * self.slots


def dot(a, b, dims=NN):
    return lax.dot_general(a, b, dims, preferred_element_type=F32)


def split(value):
    high = value.astype(BF16)
    low = (value - high.astype(F32)).astype(BF16)
    return high, low


def both(value):
    return jnp.concatenate(split(value), axis=1)


def exact_dot(onehot, value):
    width = value.shape[1]
    out = dot(onehot, both(value))
    return out[:, :width] + out[:, width:]


def iota(shape, axis):
    return lax.broadcasted_iota(jnp.int32, shape, axis)


def fiota(shape, axis):
    return iota(shape, axis).astype(F32)


def total(value):
    return jnp.sum(jnp.sum(value, axis=0, keepdims=True), axis=1, keepdims=True)


def lane_row(values):
    lane = iota((1, 128), 1)
    row = jnp.zeros((1, 128), F32)
    for index, value in enumerate(values):
        row = jnp.where(lane == index, value, row)
    return row


def lane_values(row, count):
    return [jnp.broadcast_to(row[:, i : i + 1], (1, 128)) for i in range(count)]


def store_tile(tiles_ref, index, tile):
    width = tile.shape[0]
    high, low = split(tile.T)
    base = 2 * width * index
    tiles_ref[base : base + width, :] = high
    tiles_ref[base + width : base + 2 * width, :] = low


def tile_inputs(source_index, source):
    rows = source_index.shape[0]
    width = source.shape[1]
    onehot = (fiota((rows, source.shape[0]), 1) == source_index).astype(BF16)
    out = dot(onehot, both(source))
    odd = (iota((rows, width), 0) & 1) == 1
    picked = jnp.where(odd, out[:, width:], out[:, :width]).astype(BF16)
    return jnp.concatenate([picked, picked], axis=1)


def octet_products(tiles_ref, inputs, octet, count):
    width = inputs.shape[1] // 2
    left = inputs[2 * OCTET * octet : 2 * OCTET * (octet + 1), :]
    sub = iota((2 * OCTET, width), 0)
    acc = jnp.zeros((2 * OCTET, width), F32)
    for j in range(OCTET // 2):
        tile = OCTET * octet + 2 * j
        if tile >= count:
            break
        pair = [
            tiles_ref[2 * width * t : 2 * width * (t + 1), :]
            for t in range(tile, min(tile + 2, count))
        ]
        out = dot(left, jnp.concatenate(pair, axis=1))
        for i in range(len(pair)):
            mine = (sub >> 1) == 2 * j + i
            acc = jnp.where(mine, out[:, i * width : (i + 1) * width], acc)
    return acc


def tile_products(tiles_ref, inputs, count):
    octets = inputs.shape[0] // (2 * OCTET)
    return jnp.concatenate(
        [octet_products(tiles_ref, inputs, o, count) for o in range(octets)], axis=0
    )


def sum_products(targets, count, products):
    select = (fiota((count, products.shape[0]), 0) == targets).astype(BF16)
    return exact_dot(select, products)


def every(ref, start, count, step):
    return ref[pl.ds(start, count, stride=step), :]


def prepare_kernel(
    z,
    rows_hbm,
    rows_2d_hbm,
    cols_2d_hbm,
    defect_hbm,
    mass_hbm,
    coupling_hbm,
    diag_hbm,
    send_ref,
    far_ref,
    row_meta_ref,
    near_meta_ref,
    far_meta_ref,
    own_ref,
    ids_out,
    tiles_ref,
    diag_ref,
    ids_ref,
    rows_smem,
    rows_ref,
    cols_ref,
    defect_ref,
    mass_ref,
    index,
    small_sems,
    sems,
):
    me = lax.axis_index("blk")
    base = me * z.rows
    width = z.width
    small = [
        pltpu.make_async_copy(source, target, small_sems.at[i])
        for i, (source, target) in enumerate(
            [
                (rows_hbm, rows_smem),
                (rows_2d_hbm, rows_ref),
                (cols_2d_hbm, cols_ref),
                (defect_hbm, defect_ref),
            ]
        )
    ]
    for copy in small:
        copy.start()
    zero = (me * 7 + 3) // (7 * z.devices + 5)
    chunks = []
    for i, start in enumerate(range(0, z.tiles, CHUNK)):
        part = pl.ds(start + zero, min(CHUNK, z.tiles - start))
        chunks.append(
            pltpu.make_async_copy(
                coupling_hbm.at[part], tiles_ref.at[part], sems.at[i]
            )
        )
    diag_copy = pltpu.make_async_copy(diag_hbm, diag_ref, sems.at[len(chunks)])
    mass_copy = pltpu.make_async_copy(mass_hbm, mass_ref, small_sems.at[4])
    for copy in chunks + [diag_copy, mass_copy]:
        copy.start()
    own_ref[...] = jnp.zeros_like(own_ref)
    index[...] = jnp.full(index.shape, -1, jnp.int32)
    small[0].wait()

    near = jnp.int32(0)
    far = jnp.int32(0)
    for t in range(z.tiles):
        row = rows_smem[t]
        here = ((row >= base) & (row < base + z.rows)).astype(jnp.int32)
        ids_ref[near] = jnp.int32(t)
        ids_ref[z.half + 1 + far] = jnp.int32(t)
        near = near + here
        far = far + 1 - here

    ids_copy = pltpu.make_async_copy(ids_ref, ids_out, small_sems.at[5])
    ids_copy.start()
    for copy in small[1:]:
        copy.wait()
    own_ref[0, 0 : z.rows, :] = defect_ref[...]
    defect = own_ref[0]

    count = index.shape[1]
    index[0:1, 0 : z.tiles] = rows_ref[...]
    index[1:2, 0 : z.tiles] = cols_ref[...]
    rows = index[0:1, :].astype(F32)
    cols = index[1:2, :].astype(F32)
    valid = rows >= 0
    row_owner = jnp.floor((rows + 0.5) * (1.0 / z.rows))
    col_owner = jnp.floor((cols + 0.5) * (1.0 / z.rows))
    row_local = rows - row_owner * z.rows
    col_local = cols - col_owner * z.rows
    mine = me.astype(F32)
    is_far = valid & (row_owner != mine)
    is_near = valid & (row_owner == mine)
    far_owner = jnp.where(is_far, row_owner, col_owner)
    far_local = jnp.where(is_far, row_local, col_local)
    own_local = jnp.where(is_far, col_local, row_local)
    kind = jnp.where(is_far, 1.0, jnp.where(is_near, 0.0, -1.0))
    key = jnp.where(valid, kind * z.devices + far_owner, -1.0)
    square = (count, count)
    before = iota(square, 0) < iota(square, 1)

    def ranks(value):
        wide = jnp.broadcast_to(value, square)
        same = (wide.T == wide) & before
        return jnp.sum(same.astype(F32), axis=0, keepdims=True)

    slot = ranks(key)
    position = ranks(kind)
    facts = jnp.concatenate(
        [
            far_owner,
            far_local,
            own_local,
            slot,
            jnp.ones((1, count), F32),
            jnp.zeros((3, count), F32),
        ],
        axis=0,
    )
    facts = jnp.where(valid, facts, 0.0).astype(BF16)

    def listed(members, rows_in_list):
        tile = (iota((rows_in_list, count), 0) >> 1).astype(F32)
        pick = ((position == tile) & members).astype(BF16)
        return dot(facts, pick, NT), dot(pick, facts, NT)

    near_row, near_col = listed(is_near, z.near_rows)
    far_row, far_col = listed(is_far, z.far_rows)

    place_row = (iota((1, z.near_rows), 1) >> 1).astype(F32) - z.half
    diag_row = (place_row >= 0) & (place_row < z.rows)
    near_target = jnp.where(near_row[4:5, :] > 0, near_row[2:3, :], -1.0)
    near_target = jnp.where(diag_row, place_row, near_target)
    far_target = far_row[3:4, :] * z.devices + far_row[0:1, :]
    far_target = jnp.where(far_row[4:5, :] > 0, far_target, -1.0)
    row_meta_ref[...] = jnp.full(row_meta_ref.shape, -1.0, F32)
    row_meta_ref[0:1, 0 : z.near_rows] = near_target
    row_meta_ref[1:2, 0 : z.far_rows] = far_target

    place_col = (iota((z.near_rows, 1), 0) >> 1).astype(F32) - z.half
    diag_col = (place_col >= 0) & (place_col < z.rows)
    real = near_col[:, 4:5] > 0
    first_source = near_col[:, 0:1] * z.first_rows + near_col[:, 1:2]
    first_source = jnp.where(real, first_source, -1.0)
    first_source = jnp.where(diag_col, mine * z.first_rows + place_col, first_source)
    later_source = near_col[:, 0:1] * z.send_rows + near_col[:, 3:4]
    later_source = jnp.where(real, later_source, -1.0)
    later_source = jnp.where(
        diag_col, z.devices * z.send_rows + place_col, later_source
    )
    lane = iota((z.near_rows, 128), 1)
    near_meta_ref[...] = jnp.where(lane == 0, first_source, later_source)
    far_source = jnp.where(far_col[:, 4:5] > 0, far_col[:, 2:3], -1.0)
    far_meta_ref[...] = jnp.broadcast_to(far_source, (z.far_rows, 128))

    def told(row_facts, col_facts, offset):
        shape = (col_facts.shape[0], 128)
        once = (iota(shape, 0) & 1) == 0
        match = (fiota(shape, 1) == col_facts[:, 3:4] + offset) & once
        told_value = jnp.where(match & (col_facts[:, 4:5] > 0), col_facts[:, 1:2] + 1.0, 0.0)
        owner = fiota((z.devices, row_facts.shape[1]), 0)
        return dot((owner == row_facts[0:1, :]).astype(BF16), told_value.astype(BF16))

    info = told(near_row, near_col, 0) + told(far_row, far_col, z.slots)
    for r in range(z.rows):
        send_ref[pl.ds(r, z.devices, stride=z.first_rows), :] = jnp.broadcast_to(
            defect[r : r + 1, :], (z.devices, width)
        )
    send_ref[pl.ds(z.info_row, z.devices, stride=z.first_rows), :] = info

    inputs = tile_inputs(far_source, defect)
    arrived = 0
    parts = []
    for octet in range(z.far_rows // (2 * OCTET)):
        group = range(OCTET * octet, min(OCTET * (octet + 1), z.half))
        needed = min(-(-(z.half + group[-1] + 1) // CHUNK), len(chunks))
        while arrived < needed:
            chunks[arrived].wait()
            arrived += 1
        for k in group:
            store_tile(far_ref, k, tiles_ref[ids_ref[z.half + 1 + k]])
        parts.append(octet_products(far_ref, inputs, octet, z.half))
    while arrived < len(chunks):
        chunks[arrived].wait()
        arrived += 1
    pushes = sum_products(far_target, z.cells, jnp.concatenate(parts, axis=0))
    for s in range(z.slots):
        send_ref[pl.ds(z.rows + s, z.devices, stride=z.first_rows), :] = pushes[
            s * z.devices : (s + 1) * z.devices
        ]
    ids_copy.wait()
    mass_copy.wait()
    own_ref[1, 0 : z.rows, :] = mass_ref[...]
    diag_copy.wait()


def fill_send(z, send_ref, ask_ref, far_ref, far_source, far_target, vector, dots):
    asked = exact_dot(ask_ref[...], vector)
    for s in range(z.slots):
        send_ref[pl.ds(s, z.devices, stride=z.send_rows), :] = asked[
            s * z.devices : (s + 1) * z.devices
        ]
    send_ref[pl.ds(z.dots_row, z.devices, stride=z.send_rows), :] = jnp.broadcast_to(
        lane_row(dots), (z.devices, 128)
    )
    inputs = tile_inputs(far_source, vector)
    products = tile_products(far_ref, inputs, z.half)
    pushes = sum_products(far_target, z.cells, products)
    for s in range(z.slots):
        send_ref[pl.ds(z.slots + s, z.devices, stride=z.send_rows), :] = pushes[
            s * z.devices : (s + 1) * z.devices
        ]


def landed(z, received_ref, land, start, step):
    received = [every(received_ref, start + s, z.devices, step) for s in range(z.slots)]
    return exact_dot(land, jnp.concatenate(received, axis=0))


def first_kernel(
    z,
    received_ref,
    tiles_ref,
    diag_ref,
    far_ref,
    own_ref,
    row_meta_ref,
    near_meta_ref,
    far_meta_ref,
    ids_in,
    send_ref,
    near_ref,
    state_ref,
    ask_ref,
    land_ref,
    scalar_ref,
    ids_ref,
    ids_sem,
):
    width = z.width
    ids_copy = pltpu.make_async_copy(ids_in, ids_ref, ids_sem)
    ids_copy.start()
    defect = own_ref[0]
    mass = own_ref[1]
    squares = jnp.zeros((z.devices, width), F32)
    for r in range(z.rows):
        block = every(received_ref, r, z.devices, z.first_rows)
        squares = squares + block * block
    beta_square = total(squares)
    scale = -lax.rsqrt(beta_square)
    scalar_ref[...] = jnp.broadcast_to(jnp.sqrt(beta_square), scalar_ref.shape)

    info = every(received_ref, z.info_row, z.devices, z.first_rows)
    ask, land = [], []
    for s in range(z.slots):
        lanes = fiota((z.devices, 128), 1)
        ask.append((lanes == info[:, s : s + 1] - 1.0).astype(F32))
        land.append(
            (lanes == info[:, z.slots + s : z.slots + s + 1] - 1.0).astype(F32)
        )
    ask_ref[...] = jnp.concatenate(ask, axis=0)[:, : z.padded].astype(BF16)
    land_mark = jnp.concatenate(land, axis=0).T[: z.padded, :].astype(BF16)
    land_ref[...] = land_mark

    inputs = tile_inputs(near_meta_ref[:, 0:1], received_ref[...])
    octets = z.near_rows // (2 * OCTET)
    parts = [None] * octets
    waited = False
    for octet in sorted(range(octets), key=lambda o: o < z.half // OCTET):
        for k in range(OCTET * octet, min(OCTET * (octet + 1), z.near)):
            if k < z.half and not waited:
                ids_copy.wait()
                waited = True
            tile = tiles_ref[ids_ref[k]] if k < z.half else diag_ref[k - z.half]
            store_tile(near_ref, k, tile)
        parts[octet] = octet_products(near_ref, inputs, octet, z.near)
    products = jnp.concatenate(parts, axis=0)
    image = mass * defect
    image = image + landed(z, received_ref, land_mark, z.rows, z.first_rows)
    image = image + sum_products(
        row_meta_ref[0:1, : z.near_rows], z.padded, products
    )
    v0 = defect * scale
    w0 = image * scale
    dots = [total(w0 * v0), total(w0 * w0)]
    state_ref[0] = v0
    state_ref[1] = w0
    fill_send(
        z,
        send_ref,
        ask_ref,
        far_ref,
        far_meta_ref[:, 0:1],
        row_meta_ref[1:2, : z.far_rows],
        w0,
        dots,
    )


def apply_received(
    z, received_ref, near_ref, own_ref, row_meta_ref, near_meta_ref, land_ref, vector
):
    source = jnp.concatenate([received_ref[...], vector], axis=0)
    inputs = tile_inputs(near_meta_ref[:, 1:2], source)
    products = tile_products(near_ref, inputs, z.near)
    image = own_ref[1] * vector
    image = image + landed(z, received_ref, land_ref[...], z.slots, z.send_rows)
    return image + sum_products(row_meta_ref[0:1, : z.near_rows], z.padded, products)


def second_kernel(
    z,
    received_ref,
    near_ref,
    far_ref,
    own_ref,
    row_meta_ref,
    near_meta_ref,
    far_meta_ref,
    ask_ref,
    land_ref,
    state_in,
    scalar_in,
    send_ref,
    state_ref,
    scalar_ref,
):
    v0 = state_in[0]
    w0 = state_in[1]
    received_dots = every(received_ref, z.dots_row, z.devices, z.send_rows)
    sums = jnp.sum(received_dots, axis=0, keepdims=True)
    h00, g00 = lane_values(sums, 2)
    inverse = lax.rsqrt(jnp.maximum(g00 - h00 * h00, FLOOR * g00))
    v1 = (w0 - h00 * v0) * inverse
    image = apply_received(
        z, received_ref, near_ref, own_ref, row_meta_ref, near_meta_ref, land_ref, w0
    )
    w1 = (image - h00 * w0) * inverse
    dots = [total(w1 * v0), total(w1 * v1), total(w1 * w1), total(w1 * w0)]
    state_ref[0] = v0
    state_ref[1] = v1
    state_ref[2] = w0
    state_ref[3] = w1
    scalar_ref[...] = jnp.broadcast_to(
        lane_row([scalar_in[0:1, 0:1], h00, g00]), scalar_ref.shape
    )
    fill_send(
        z,
        send_ref,
        ask_ref,
        far_ref,
        far_meta_ref[:, 0:1],
        row_meta_ref[1:2, : z.far_rows],
        w1,
        dots,
    )


def third_kernel(
    z,
    received_ref,
    near_ref,
    own_ref,
    row_meta_ref,
    near_meta_ref,
    land_ref,
    state_in,
    scalar_in,
    send_ref,
    state_ref,
    scalar_ref,
):
    v0, v1, w0, w1 = state_in[0], state_in[1], state_in[2], state_in[3]
    received_dots = every(received_ref, z.dots_row, z.devices, z.send_rows)
    sums = jnp.sum(received_dots, axis=0, keepdims=True)
    h01, h11, g11, g01 = lane_values(sums, 4)
    inverse = lax.rsqrt(jnp.maximum(g11 - h01 * h01 - h11 * h11, FLOOR * g11))
    v2 = (w1 - h01 * v0 - h11 * v1) * inverse
    beta, h00, g00 = lane_values(scalar_in[0:1, :], 3)
    i00 = lax.rsqrt(g00)
    l10 = g01 * i00
    i11 = lax.rsqrt(g11 - l10 * l10)
    f0 = beta * h00 * i00
    f1 = (beta * h01 - l10 * f0) * i11
    image = apply_received(
        z, received_ref, near_ref, own_ref, row_meta_ref, near_meta_ref, land_ref, w1
    )
    w2 = (image - h01 * w0 - h11 * w1) * inverse
    dots = [total(w2 * v0), total(w2 * w0), total(w2 * w1), total(w2 * w2)]
    state_ref[0] = v0
    state_ref[1] = v1
    state_ref[2] = v2
    for row, value in enumerate([beta, i00, l10, i11, f0, f1]):
        scalar_ref[row : row + 1, :] = value
    send_ref[...] = jnp.broadcast_to(lane_row(dots), (z.devices, 128))


def last_kernel(z, received_ref, state_in, scalar_in, out_ref):
    sums = jnp.sum(received_ref[...], axis=0, keepdims=True)
    d, g02, g12, g22 = lane_values(sums, 4)
    beta, i00, l10, i11, f0, f1 = [scalar_in[row : row + 1, :] for row in range(6)]
    l20 = g02 * i00
    l21 = (g12 - l20 * l10) * i11
    y2 = (beta * d - l20 * f0 - l21 * f1) / (g22 - l20 * l20 - l21 * l21)
    y1 = (f1 - l21 * y2) * i11
    y0 = (f0 - l10 * y1 - l20 * y2) * i00
    update = y0 * state_in[0] + y1 * state_in[1] + y2 * state_in[2]
    out_ref[...] = update[0 : z.rows, :]


def exchange(z, value):
    rows, width = value.shape
    value = value.reshape(z.devices, 1, rows // z.devices * width)
    value = lax.all_to_all(value, "blk", split_axis=0, concat_axis=0, tiled=True)
    return value.reshape(rows, width)


def on_device(defect, mass, block_diag, coupling, tile_rows, tile_cols):
    z = Sizes(lax.axis_size("blk"), defect.shape[0], defect.shape[1], tile_rows.shape[0])
    width = z.width
    vmem = pl.BlockSpec(memory_space=pltpu.VMEM)
    hbm = pl.BlockSpec(memory_space=pltpu.HBM)

    def shape(*dims, dtype=F32):
        return jax.ShapeDtypeStruct(dims, dtype)

    def in_hbm(value):
        return pltpu.with_memory_space_constraint(value, pltpu.HBM)

    def call(kernel, name, ins, outs, scratch, args, limit=4):
        return pl.pallas_call(
            functools.partial(kernel, z),
            out_shape=outs,
            in_specs=ins,
            out_specs=[vmem] * len(outs),
            scratch_shapes=scratch,
            name=name,
            compiler_params=pltpu.CompilerParams(vmem_limit_bytes=limit * MIB),
        )(*args)

    def pieces(count):
        return shape(2 * count * width, width, dtype=BF16)

    rows_2d = tile_rows.reshape(1, z.tiles)
    cols_2d = tile_cols.reshape(1, z.tiles)
    send, far, row_meta, near_meta, far_meta, own, ids, tiles, diag = call(
        prepare_kernel,
        "prepare",
        [hbm] * 7,
        [
            shape(z.devices * z.first_rows, width),
            pieces(z.half),
            shape(8, round_up(max(z.near_rows, z.far_rows), 128)),
            shape(z.near_rows, 128),
            shape(z.far_rows, 128),
            shape(2, z.padded, width),
            shape(2 * z.half + 2, dtype=jnp.int32),
            shape(z.tiles, width, width),
            shape(z.rows, width, width),
        ],
        [
            pltpu.SMEM((2 * z.half + 2,), jnp.int32),
            pltpu.SMEM((z.tiles,), jnp.int32),
            pltpu.VMEM((1, z.tiles), jnp.int32),
            pltpu.VMEM((1, z.tiles), jnp.int32),
            pltpu.VMEM((z.rows, width), F32),
            pltpu.VMEM((z.rows, width), F32),
            pltpu.VMEM((8, round_up(z.tiles, 128)), jnp.int32),
            pltpu.SemaphoreType.DMA((6,)),
            pltpu.SemaphoreType.DMA((-(-z.tiles // CHUNK) + 1,)),
        ],
        map(in_hbm, (tile_rows, rows_2d, cols_2d, defect, mass, coupling, block_diag)),
    )
    received = exchange(z, send)
    send, near, state, ask, land, scalars = call(
        first_kernel,
        "first",
        [vmem] * 9,
        [
            shape(z.devices * z.send_rows, width),
            pieces(z.near),
            shape(2, z.padded, width),
            shape(z.cells, z.padded, dtype=BF16),
            shape(z.padded, z.cells, dtype=BF16),
            shape(8, 128),
        ],
        [pltpu.SMEM((2 * z.half + 2,), jnp.int32), pltpu.SemaphoreType.DMA],
        (received, tiles, diag, far, own, row_meta, near_meta, far_meta, ids),
    )
    received = exchange(z, send)
    send, state, scalars = call(
        second_kernel,
        "second",
        [vmem] * 11,
        [
            shape(z.devices * z.send_rows, width),
            shape(4, z.padded, width),
            shape(8, 128),
        ],
        [],
        (
            received,
            near,
            far,
            own,
            row_meta,
            near_meta,
            far_meta,
            ask,
            land,
            state,
            scalars,
        ),
    )
    received = exchange(z, send)
    send, state, scalars = call(
        third_kernel,
        "third",
        [vmem] * 8,
        [
            shape(z.devices, width),
            shape(3, z.padded, width),
            shape(8, 128),
        ],
        [],
        (received, near, own, row_meta, near_meta, land, state, scalars),
    )
    received = exchange(z, send)
    (update,) = call(
        last_kernel,
        "last",
        [vmem] * 3,
        [shape(z.rows, width)],
        [],
        (received, state, scalars),
    )
    return update


def solution(mesh):
    in_specs = (
        P("blk", None),
        P("blk", None),
        P("blk", None, None),
        P("blk", None, None),
        P("blk"),
        P("blk"),
    )
    return jax.shard_map(
        on_device, mesh=mesh, in_specs=in_specs, out_specs=P("blk", None), check_vma=False
    )
```

```python
import functools

import jax
import jax.numpy as jnp
from jax import lax
from jax.experimental import pallas as pl
from jax.experimental.pallas import tpu as pltpu
from jax.sharding import PartitionSpec as P

F32 = jnp.float32
BF16 = jnp.bfloat16
NT = (((1,), (1,)), ((), ()))
NN = (((1,), (0,)), ((), ()))
FLOOR = 2.0**-22
MIB = 1 << 20
CHUNK = 32
OCTET = 8


def round_up(value, step):
    return -(-value // step) * step


class Sizes:
    def __init__(self, devices, rows, width, tiles):
        self.devices = devices
        self.rows = rows
        self.width = width
        self.tiles = tiles
        self.half = tiles // 2
        self.near = self.half + rows
        self.slots = (self.half + devices - 2) // (devices - 1)
        self.cells = self.slots * devices
        self.padded = round_up(rows, 16)
        self.near_rows = 2 * round_up(self.near, OCTET)
        self.far_rows = 2 * round_up(self.half, OCTET)
        self.first_rows = rows + self.slots + 1
        self.info_row = rows + self.slots
        self.send_rows = 2 * self.slots + 1
        self.dots_row = 2 * self.slots


def dot(a, b, dims=NN):
    return lax.dot_general(a, b, dims, preferred_element_type=F32)


def split(value):
    high = value.astype(BF16)
    low = (value - high.astype(F32)).astype(BF16)
    return high, low


def both(value):
    return jnp.concatenate(split(value), axis=1)


def exact_dot(onehot, value):
    width = value.shape[1]
    out = dot(onehot, both(value))
    return out[:, :width] + out[:, width:]


def iota(shape, axis):
    return lax.broadcasted_iota(jnp.int32, shape, axis)


def fiota(shape, axis):
    return iota(shape, axis).astype(F32)


def total(value):
    return jnp.sum(jnp.sum(value, axis=0, keepdims=True), axis=1, keepdims=True)


def lane_row(values):
    lane = iota((1, 128), 1)
    row = jnp.zeros((1, 128), F32)
    for index, value in enumerate(values):
        row = jnp.where(lane == index, value, row)
    return row


def lane_values(row, count):
    return [jnp.broadcast_to(row[:, i : i + 1], (1, 128)) for i in range(count)]


def store_tile(tiles_ref, index, tile):
    width = tile.shape[0]
    high, low = split(tile.T)
    base = 2 * width * index
    tiles_ref[base : base + width, :] = high
    tiles_ref[base + width : base + 2 * width, :] = low


def tile_inputs(source_index, source):
    rows = source_index.shape[0]
    width = source.shape[1]
    onehot = (fiota((rows, source.shape[0]), 1) == source_index).astype(BF16)
    out = dot(onehot, both(source))
    odd = (iota((rows, width), 0) & 1) == 1
    picked = jnp.where(odd, out[:, width:], out[:, :width]).astype(BF16)
    return jnp.concatenate([picked, picked], axis=1)


def octet_products(tiles_ref, inputs, octet, count):
    width = inputs.shape[1] // 2
    left = inputs[2 * OCTET * octet : 2 * OCTET * (octet + 1), :]
    sub = iota((2 * OCTET, width), 0)
    acc = jnp.zeros((2 * OCTET, width), F32)
    for j in range(OCTET // 2):
        tile = OCTET * octet + 2 * j
        if tile >= count:
            break
        pair = [
            tiles_ref[2 * width * t : 2 * width * (t + 1), :]
            for t in range(tile, min(tile + 2, count))
        ]
        out = dot(left, jnp.concatenate(pair, axis=1))
        for i in range(len(pair)):
            mine = (sub >> 1) == 2 * j + i
            acc = jnp.where(mine, out[:, i * width : (i + 1) * width], acc)
    return acc


def tile_products(tiles_ref, inputs, count):
    octets = inputs.shape[0] // (2 * OCTET)
    return jnp.concatenate(
        [octet_products(tiles_ref, inputs, o, count) for o in range(octets)], axis=0
    )


def sum_products(targets, count, products):
    select = (fiota((count, products.shape[0]), 0) == targets).astype(BF16)
    return exact_dot(select, products)


def every(ref, start, count, step):
    return ref[pl.ds(start, count, stride=step), :]


def prepare_kernel(
    z,
    rows_hbm,
    rows_2d_hbm,
    cols_2d_hbm,
    defect_hbm,
    mass_hbm,
    coupling_hbm,
    diag_hbm,
    send_ref,
    far_ref,
    row_meta_ref,
    near_meta_ref,
    far_meta_ref,
    own_ref,
    near_list_ref,
    tiles_ref,
    ids_ref,
    rows_smem,
    rows_ref,
    cols_ref,
    defect_ref,
    mass_ref,
    index,
    small_sems,
    sems,
):
    me = lax.axis_index("blk")
    base = me * z.rows
    width = z.width
    small = [
        pltpu.make_async_copy(source, target, small_sems.at[i])
        for i, (source, target) in enumerate(
            [
                (rows_hbm, rows_smem),
                (rows_2d_hbm, rows_ref),
                (cols_2d_hbm, cols_ref),
                (defect_hbm, defect_ref),
            ]
        )
    ]
    for copy in small:
        copy.start()
    zero = (me * 7 + 3) // (7 * z.devices + 5)
    chunks = []
    for i, start in enumerate(range(0, z.tiles, CHUNK)):
        part = pl.ds(start + zero, min(CHUNK, z.tiles - start))
        chunks.append(
            pltpu.make_async_copy(
                coupling_hbm.at[part], tiles_ref.at[part], sems.at[i]
            )
        )
    diag_copy = pltpu.make_async_copy(
        diag_hbm, near_list_ref.at[pl.ds(z.half, z.rows)], sems.at[len(chunks)]
    )
    mass_copy = pltpu.make_async_copy(mass_hbm, mass_ref, small_sems.at[4])
    for copy in chunks + [diag_copy, mass_copy]:
        copy.start()
    own_ref[...] = jnp.zeros_like(own_ref)
    index[...] = jnp.full(index.shape, -1, jnp.int32)
    small[0].wait()

    near = jnp.int32(0)
    for t in range(z.tiles):
        offset = rows_smem[t] - base
        here = (offset >= 0) & (offset < z.rows)
        ids_ref[jnp.where(here, near, z.half + t - near)] = jnp.int32(t)
        near = near + here.astype(jnp.int32)
    for copy in small[1:]:
        copy.wait()
    own_ref[0, 0 : z.rows, :] = defect_ref[...]
    defect = own_ref[0]

    count = index.shape[1]
    index[0:1, 0 : z.tiles] = rows_ref[...]
    index[1:2, 0 : z.tiles] = cols_ref[...]
    rows = index[0:1, :].astype(F32)
    cols = index[1:2, :].astype(F32)
    valid = rows >= 0
    row_owner = jnp.floor((rows + 0.5) * (1.0 / z.rows))
    col_owner = jnp.floor((cols + 0.5) * (1.0 / z.rows))
    row_local = rows - row_owner * z.rows
    col_local = cols - col_owner * z.rows
    mine = me.astype(F32)
    is_far = valid & (row_owner != mine)
    is_near = valid & (row_owner == mine)
    far_owner = jnp.where(is_far, row_owner, col_owner)
    far_local = jnp.where(is_far, row_local, col_local)
    own_local = jnp.where(is_far, col_local, row_local)
    kind = jnp.where(is_far, 1.0, jnp.where(is_near, 0.0, -1.0))
    key = jnp.where(valid, kind * z.devices + far_owner, -1.0)
    square = (count, count)
    before = iota(square, 0) < iota(square, 1)

    def ranks(value):
        wide = jnp.broadcast_to(value, square)
        same = (wide.T == wide) & before
        return jnp.sum(same.astype(F32), axis=0, keepdims=True)

    slot = ranks(key)
    position = ranks(kind)
    facts = jnp.concatenate(
        [
            far_owner,
            far_local,
            own_local,
            slot,
            jnp.ones((1, count), F32),
            jnp.zeros((3, count), F32),
        ],
        axis=0,
    )
    facts = jnp.where(valid, facts, 0.0).astype(BF16)

    def listed(members, rows_in_list):
        tile = (iota((rows_in_list, count), 0) >> 1).astype(F32)
        pick = ((position == tile) & members).astype(BF16)
        return dot(facts, pick, NT), dot(pick, facts, NT)

    far_row, far_col = listed(is_far, z.far_rows)
    far_source = jnp.where(far_col[:, 4:5] > 0, far_col[:, 2:3], -1.0)
    far_target = far_row[3:4, :] * z.devices + far_row[0:1, :]
    far_target = jnp.where(far_row[4:5, :] > 0, far_target, -1.0)
    far_meta_ref[...] = jnp.broadcast_to(far_source, (z.far_rows, 128))

    def describe():
        near_row, near_col = listed(is_near, z.near_rows)

        place_row = (iota((1, z.near_rows), 1) >> 1).astype(F32) - z.half
        diag_row = (place_row >= 0) & (place_row < z.rows)
        near_target = jnp.where(near_row[4:5, :] > 0, near_row[2:3, :], -1.0)
        near_target = jnp.where(diag_row, place_row, near_target)
        row_meta_ref[...] = jnp.full(row_meta_ref.shape, -1.0, F32)
        row_meta_ref[0:1, 0 : z.near_rows] = near_target
        row_meta_ref[1:2, 0 : z.far_rows] = far_target

        place_col = (iota((z.near_rows, 1), 0) >> 1).astype(F32) - z.half
        diag_col = (place_col >= 0) & (place_col < z.rows)
        real = near_col[:, 4:5] > 0
        first_source = near_col[:, 0:1] * z.first_rows + near_col[:, 1:2]
        first_source = jnp.where(real, first_source, -1.0)
        first_source = jnp.where(diag_col, mine * z.first_rows + place_col, first_source)
        later_source = near_col[:, 0:1] * z.send_rows + near_col[:, 3:4]
        later_source = jnp.where(real, later_source, -1.0)
        later_source = jnp.where(
            diag_col, z.devices * z.send_rows + place_col, later_source
        )
        lane = iota((z.near_rows, 128), 1)
        near_meta_ref[...] = jnp.where(lane == 0, first_source, later_source)

        def told(row_facts, col_facts, offset):
            shape = (col_facts.shape[0], 128)
            once = (iota(shape, 0) & 1) == 0
            match = (fiota(shape, 1) == col_facts[:, 3:4] + offset) & once
            told_value = jnp.where(match & (col_facts[:, 4:5] > 0), col_facts[:, 1:2] + 1.0, 0.0)
            owner = fiota((z.devices, row_facts.shape[1]), 0)
            return dot((owner == row_facts[0:1, :]).astype(BF16), told_value.astype(BF16))

        info = told(near_row, near_col, 0) + told(far_row, far_col, z.slots)
        for r in range(z.rows):
            send_ref[pl.ds(r, z.devices, stride=z.first_rows), :] = jnp.broadcast_to(
                defect[r : r + 1, :], (z.devices, width)
            )
        send_ref[pl.ds(z.info_row, z.devices, stride=z.first_rows), :] = info


    describe()
    inputs = tile_inputs(far_source, defect)
    arrived = 0
    parts = []
    for octet in range(z.far_rows // (2 * OCTET)):
        group = range(OCTET * octet, min(OCTET * (octet + 1), z.half))
        needed = min(-(-(z.half + group[-1] + 1) // CHUNK), len(chunks))
        while arrived < needed:
            chunks[arrived].wait()
            arrived += 1
        for k in group:
            store_tile(far_ref, k, tiles_ref[ids_ref[z.half + k]])
            near_list_ref[k] = tiles_ref[ids_ref[k]]
        parts.append(octet_products(far_ref, inputs, octet, z.half))
    while arrived < len(chunks):
        chunks[arrived].wait()
        arrived += 1
    pushes = sum_products(far_target, z.cells, jnp.concatenate(parts, axis=0))
    for s in range(z.slots):
        send_ref[pl.ds(z.rows + s, z.devices, stride=z.first_rows), :] = pushes[
            s * z.devices : (s + 1) * z.devices
        ]
    mass_copy.wait()
    own_ref[1, 0 : z.rows, :] = mass_ref[...]
    diag_copy.wait()


def fill_send(z, send_ref, ask_ref, far_ref, far_source, far_target, vector, dots):
    asked = exact_dot(ask_ref[...], vector)
    for s in range(z.slots):
        send_ref[pl.ds(s, z.devices, stride=z.send_rows), :] = asked[
            s * z.devices : (s + 1) * z.devices
        ]
    send_ref[pl.ds(z.dots_row, z.devices, stride=z.send_rows), :] = jnp.broadcast_to(
        lane_row(dots), (z.devices, 128)
    )
    inputs = tile_inputs(far_source, vector)
    products = tile_products(far_ref, inputs, z.half)
    pushes = sum_products(far_target, z.cells, products)
    for s in range(z.slots):
        send_ref[pl.ds(z.slots + s, z.devices, stride=z.send_rows), :] = pushes[
            s * z.devices : (s + 1) * z.devices
        ]


def landed(z, received_ref, land, start, step):
    received = [every(received_ref, start + s, z.devices, step) for s in range(z.slots)]
    return exact_dot(land, jnp.concatenate(received, axis=0))


def first_kernel(
    z,
    received_ref,
    near_list_ref,
    far_ref,
    own_ref,
    row_meta_ref,
    near_meta_ref,
    far_meta_ref,
    send_ref,
    near_ref,
    state_ref,
    ask_ref,
    land_ref,
    scalar_ref,
):
    width = z.width
    defect = own_ref[0]
    mass = own_ref[1]
    squares = jnp.zeros((z.devices, width), F32)
    for r in range(z.rows):
        block = every(received_ref, r, z.devices, z.first_rows)
        squares = squares + block * block
    beta_square = total(squares)
    scale = -lax.rsqrt(beta_square)
    scalar_ref[...] = jnp.broadcast_to(jnp.sqrt(beta_square), scalar_ref.shape)

    info = every(received_ref, z.info_row, z.devices, z.first_rows)
    ask, land = [], []
    for s in range(z.slots):
        lanes = fiota((z.devices, 128), 1)
        ask.append((lanes == info[:, s : s + 1] - 1.0).astype(F32))
        land.append(
            (lanes == info[:, z.slots + s : z.slots + s + 1] - 1.0).astype(F32)
        )
    ask_ref[...] = jnp.concatenate(ask, axis=0)[:, : z.padded].astype(BF16)
    land_mark = jnp.concatenate(land, axis=0).T[: z.padded, :].astype(BF16)
    land_ref[...] = land_mark

    inputs = tile_inputs(near_meta_ref[:, 0:1], received_ref[...])
    parts = []
    for octet in range(z.near_rows // (2 * OCTET)):
        for k in range(OCTET * octet, min(OCTET * (octet + 1), z.near)):
            store_tile(near_ref, k, near_list_ref[k])
        parts.append(octet_products(near_ref, inputs, octet, z.near))
    products = jnp.concatenate(parts, axis=0)
    image = mass * defect
    image = image + landed(z, received_ref, land_mark, z.rows, z.first_rows)
    image = image + sum_products(
        row_meta_ref[0:1, : z.near_rows], z.padded, products
    )
    v0 = defect * scale
    w0 = image * scale
    dots = [total(w0 * v0), total(w0 * w0)]
    state_ref[0] = v0
    state_ref[1] = w0
    fill_send(
        z,
        send_ref,
        ask_ref,
        far_ref,
        far_meta_ref[:, 0:1],
        row_meta_ref[1:2, : z.far_rows],
        w0,
        dots,
    )


def apply_received(
    z, received_ref, near_ref, own_ref, row_meta_ref, near_meta_ref, land_ref, vector
):
    source = jnp.concatenate([received_ref[...], vector], axis=0)
    inputs = tile_inputs(near_meta_ref[:, 1:2], source)
    products = tile_products(near_ref, inputs, z.near)
    image = own_ref[1] * vector
    image = image + landed(z, received_ref, land_ref[...], z.slots, z.send_rows)
    return image + sum_products(row_meta_ref[0:1, : z.near_rows], z.padded, products)


def second_kernel(
    z,
    received_ref,
    near_ref,
    far_ref,
    own_ref,
    row_meta_ref,
    near_meta_ref,
    far_meta_ref,
    ask_ref,
    land_ref,
    state_in,
    scalar_in,
    send_ref,
    state_ref,
    scalar_ref,
):
    v0 = state_in[0]
    w0 = state_in[1]
    received_dots = every(received_ref, z.dots_row, z.devices, z.send_rows)
    sums = jnp.sum(received_dots, axis=0, keepdims=True)
    h00, g00 = lane_values(sums, 2)
    inverse = lax.rsqrt(jnp.maximum(g00 - h00 * h00, FLOOR * g00))
    v1 = (w0 - h00 * v0) * inverse
    image = apply_received(
        z, received_ref, near_ref, own_ref, row_meta_ref, near_meta_ref, land_ref, w0
    )
    w1 = (image - h00 * w0) * inverse
    dots = [total(w1 * v0), total(w1 * v1), total(w1 * w1), total(w1 * w0)]
    state_ref[0] = v0
    state_ref[1] = v1
    state_ref[2] = w0
    state_ref[3] = w1
    scalar_ref[...] = jnp.broadcast_to(
        lane_row([scalar_in[0:1, 0:1], h00, g00]), scalar_ref.shape
    )
    fill_send(
        z,
        send_ref,
        ask_ref,
        far_ref,
        far_meta_ref[:, 0:1],
        row_meta_ref[1:2, : z.far_rows],
        w1,
        dots,
    )


def third_kernel(
    z,
    received_ref,
    near_ref,
    own_ref,
    row_meta_ref,
    near_meta_ref,
    land_ref,
    state_in,
    scalar_in,
    send_ref,
    state_ref,
    scalar_ref,
):
    v0, v1, w0, w1 = state_in[0], state_in[1], state_in[2], state_in[3]
    received_dots = every(received_ref, z.dots_row, z.devices, z.send_rows)
    sums = jnp.sum(received_dots, axis=0, keepdims=True)
    h01, h11, g11, g01 = lane_values(sums, 4)
    inverse = lax.rsqrt(jnp.maximum(g11 - h01 * h01 - h11 * h11, FLOOR * g11))
    v2 = (w1 - h01 * v0 - h11 * v1) * inverse
    beta, h00, g00 = lane_values(scalar_in[0:1, :], 3)
    i00 = lax.rsqrt(g00)
    l10 = g01 * i00
    i11 = lax.rsqrt(g11 - l10 * l10)
    f0 = beta * h00 * i00
    f1 = (beta * h01 - l10 * f0) * i11
    image = apply_received(
        z, received_ref, near_ref, own_ref, row_meta_ref, near_meta_ref, land_ref, w1
    )
    w2 = (image - h01 * w0 - h11 * w1) * inverse
    dots = [total(w2 * v0), total(w2 * w0), total(w2 * w1), total(w2 * w2)]
    state_ref[0] = v0
    state_ref[1] = v1
    state_ref[2] = v2
    for row, value in enumerate([beta, i00, l10, i11, f0, f1]):
        scalar_ref[row : row + 1, :] = value
    send_ref[...] = jnp.broadcast_to(lane_row(dots), (z.devices, 128))


def last_kernel(z, received_ref, state_in, scalar_in, out_ref):
    sums = jnp.sum(received_ref[...], axis=0, keepdims=True)
    d, g02, g12, g22 = lane_values(sums, 4)
    beta, i00, l10, i11, f0, f1 = [scalar_in[row : row + 1, :] for row in range(6)]
    l20 = g02 * i00
    l21 = (g12 - l20 * l10) * i11
    y2 = (beta * d - l20 * f0 - l21 * f1) / (g22 - l20 * l20 - l21 * l21)
    y1 = (f1 - l21 * y2) * i11
    y0 = (f0 - l10 * y1 - l20 * y2) * i00
    update = y0 * state_in[0] + y1 * state_in[1] + y2 * state_in[2]
    out_ref[...] = update[0 : z.rows, :]


def exchange(z, value):
    rows, width = value.shape
    value = value.reshape(z.devices, 1, rows // z.devices * width)
    value = lax.all_to_all(value, "blk", split_axis=0, concat_axis=0, tiled=True)
    return value.reshape(rows, width)


def on_device(defect, mass, block_diag, coupling, tile_rows, tile_cols):
    z = Sizes(lax.axis_size("blk"), defect.shape[0], defect.shape[1], tile_rows.shape[0])
    width = z.width
    vmem = pl.BlockSpec(memory_space=pltpu.VMEM)
    hbm = pl.BlockSpec(memory_space=pltpu.HBM)

    def shape(*dims, dtype=F32):
        return jax.ShapeDtypeStruct(dims, dtype)

    def in_hbm(value):
        return pltpu.with_memory_space_constraint(value, pltpu.HBM)

    def call(kernel, name, ins, outs, scratch, args, limit=4):
        return pl.pallas_call(
            functools.partial(kernel, z),
            out_shape=outs,
            in_specs=ins,
            out_specs=[vmem] * len(outs),
            scratch_shapes=scratch,
            name=name,
            compiler_params=pltpu.CompilerParams(vmem_limit_bytes=limit * MIB),
        )(*args)

    def pieces(count):
        return shape(2 * count * width, width, dtype=BF16)

    rows_2d = tile_rows.reshape(1, z.tiles)
    cols_2d = tile_cols.reshape(1, z.tiles)
    send, far, row_meta, near_meta, far_meta, own, near_list = call(
        prepare_kernel,
        "prepare",
        [hbm] * 7,
        [
            shape(z.devices * z.first_rows, width),
            pieces(z.half),
            shape(8, round_up(max(z.near_rows, z.far_rows), 128)),
            shape(z.near_rows, 128),
            shape(z.far_rows, 128),
            shape(2, z.padded, width),
            shape(z.near, width, width),
        ],
        [
            pltpu.VMEM((z.tiles, width, width), F32),
            pltpu.SMEM((z.tiles,), jnp.int32),
            pltpu.SMEM((z.tiles,), jnp.int32),
            pltpu.VMEM((1, z.tiles), jnp.int32),
            pltpu.VMEM((1, z.tiles), jnp.int32),
            pltpu.VMEM((z.rows, width), F32),
            pltpu.VMEM((z.rows, width), F32),
            pltpu.VMEM((8, round_up(z.tiles, 128)), jnp.int32),
            pltpu.SemaphoreType.DMA((5,)),
            pltpu.SemaphoreType.DMA((-(-z.tiles // CHUNK) + 1,)),
        ],
        map(in_hbm, (tile_rows, rows_2d, cols_2d, defect, mass, coupling, block_diag)),
        z.tiles * width * width * 4 // MIB + 4,
    )
    received = exchange(z, send)
    send, near, state, ask, land, scalars = call(
        first_kernel,
        "first",
        [vmem] * 7,
        [
            shape(z.devices * z.send_rows, width),
            pieces(z.near),
            shape(2, z.padded, width),
            shape(z.cells, z.padded, dtype=BF16),
            shape(z.padded, z.cells, dtype=BF16),
            shape(8, 128),
        ],
        [],
        (received, near_list, far, own, row_meta, near_meta, far_meta),
    )
    received = exchange(z, send)
    send, state, scalars = call(
        second_kernel,
        "second",
        [vmem] * 11,
        [
            shape(z.devices * z.send_rows, width),
            shape(4, z.padded, width),
            shape(8, 128),
        ],
        [],
        (
            received,
            near,
            far,
            own,
            row_meta,
            near_meta,
            far_meta,
            ask,
            land,
            state,
            scalars,
        ),
    )
    received = exchange(z, send)
    send, state, scalars = call(
        third_kernel,
        "third",
        [vmem] * 8,
        [
            shape(z.devices, width),
            shape(3, z.padded, width),
            shape(8, 128),
        ],
        [],
        (received, near, own, row_meta, near_meta, land, state, scalars),
    )
    received = exchange(z, send)
    (update,) = call(
        last_kernel,
        "last",
        [vmem] * 3,
        [shape(z.rows, width)],
        [],
        (received, state, scalars),
    )
    return update


def solution(mesh):
    in_specs = (
        P("blk", None),
        P("blk", None),
        P("blk", None, None),
        P("blk", None, None),
        P("blk"),
        P("blk"),
    )
    return jax.shard_map(
        on_device, mesh=mesh, in_specs=in_specs, out_specs=P("blk", None), check_vma=False
    )
```
